32 devices in a mesh: seg: 4 (over z), cp: 8 (over y, x, core).
Axes of the slice: x: 2, y: 2, z: 4, core: 2. Of those that a mesh axis runs over, the one named last changes fastest.
Arguments:
- mixed_qkv: bfloat16 [4096, 8192], P(('seg', 'cp')), may hold values from -6 to 6
- gate_z: bfloat16 [4096, 4096], P(('seg', 'cp')), may hold values from -6 to 6
- gate_logits: bfloat16 [4096, 64], P(('seg', 'cp')), may hold values from -16 to 4
- block_table: int32 [4, 16], P('seg'), may hold values from 0 to 15, as said below
- conv_weight: float32 [4, 8192], replicated, may hold values from -3 to 3
- a_log: float32 [32], replicated, may hold values from -0.7 to 0.7
- dt_bias: float32 [32], replicated, may hold values from -0.5 to 0.5
- norm_gain: float32 [128], replicated, may hold values from 0.25 to 1.75
Outputs:
- mixed_out: bfloat16 [4096, 4096], P(('seg', 'cp'))
The draws below stay inside these ranges and needn't reach their ends.
Inputs may be any that keep to these rules, and one draw needn't show every extreme that they name: Each row of block_table is a permutation of the numbers 0 to 15; its entries at even positions are below 8, those at odd positions are 8 or more.
All inputs are finite; a program needn't handle non-finite values.
Results may differ from the reference program's by a relative error of at most 0.001.
Values may be sent and summed in bfloat16 or wider, within the bound.
A program may use at most 128 MiB of HBM per device.

```python
import jax
import jax.numpy as jnp
from jax import lax

VALUE_HEADS = 32
KEY_HEADS = 16
HEAD_DIM = 128
CONV = 4
BLOCK = 128
TOK_DEV = 128
SEQUENCE_TOKENS = 4096
N_SEG = 4
N_CP = 8


def draw_gate_logits(key, part):
    random_subkeys = jax.random.split(key, 9)
    slow_share = 0.5
    beta_noise = 0.5 * jax.random.normal(random_subkeys[4], (SEQUENCE_TOKENS, VALUE_HEADS), jnp.float32)
    slow_heads = jax.random.uniform(random_subkeys[0], (VALUE_HEADS,), jnp.float32) < slow_share
    beta_base = jnp.where(slow_heads, jax.random.uniform(random_subkeys[1], (VALUE_HEADS,), jnp.float32, -7.0, -5.0), jax.random.uniform(random_subkeys[2], (VALUE_HEADS,), jnp.float32, -1.0, 2.0))
    decay_base = jnp.where(slow_heads, jax.random.uniform(random_subkeys[3], (VALUE_HEADS,), jnp.float32, -13.0, -11.0), jax.random.uniform(random_subkeys[5], (VALUE_HEADS,), jnp.float32, -4.0, -3.0))
    rows_per_half = TOK_DEV // 2
    group_count = SEQUENCE_TOKENS // rows_per_half
    offsets = jax.random.uniform(random_subkeys[6], (group_count, 1, VALUE_HEADS), jnp.float32, -0.7, 0.7)
    offsets = jnp.broadcast_to(offsets, (group_count, rows_per_half, VALUE_HEADS)).reshape(SEQUENCE_TOKENS, VALUE_HEADS)
    beta_logit = beta_base + beta_noise
    decay_logit_raw = decay_base + offsets + 0.3 * jax.random.normal(random_subkeys[7], (SEQUENCE_TOKENS, VALUE_HEADS), jnp.float32)
    doubling_rows = jax.random.uniform(random_subkeys[8], (SEQUENCE_TOKENS, 1), jnp.float32) < 6.0 / SEQUENCE_TOKENS
    doubling_level = jax.random.uniform(jax.random.fold_in(random_subkeys[8], 7), (SEQUENCE_TOKENS, VALUE_HEADS), jnp.float32, -1.0, 0.0)
    decay_logit_raw = jnp.where(doubling_rows, jnp.maximum(decay_logit_raw, doubling_level), decay_logit_raw)
    joined = jnp.concatenate([beta_logit, decay_logit_raw], axis=1)
    return jnp.clip(joined, -16.0, 4.0).astype(jnp.bfloat16)


def draw_block_table(key, part):
    base = jax.random.fold_in(key, 41)
    first_keys = jax.random.split(jax.random.fold_in(base, 1), N_SEG)
    second_keys = jax.random.split(jax.random.fold_in(base, 2), N_SEG)
    first = jax.vmap(lambda one: jax.random.permutation(one, N_CP))(first_keys).astype(jnp.int32)
    second = jax.vmap(lambda one: jax.random.permutation(one, N_CP))(second_keys).astype(jnp.int32) + N_CP
    return jnp.stack([first, second], axis=-1).reshape(N_SEG, 2 * N_CP).astype(jnp.int32)


def levels(own_key, shape, cuts, least, largest):
    factor_of = 1.0
    for position, blocks in cuts:
        draws = jax.random.uniform(jax.random.fold_in(jax.random.fold_in(own_key, 6), position), (blocks,), jnp.float32, least / len(cuts), largest / len(cuts))
        factor_of = factor_of * jnp.repeat(jnp.exp(draws), shape[position] // blocks).reshape((-1,) + (1,) * (len(shape) - 1 - position))
    return factor_of


def normal_values(own_key, shape, deviation, most, cuts=(), kind=jnp.bfloat16):
    factor_of = levels(own_key, shape, cuts, -0.22, 0.18) if cuts else 1.0
    values = jax.random.normal(own_key, shape, jnp.float32) * deviation * factor_of
    return jnp.minimum(jnp.maximum(values, -most), most).astype(kind)


def setup_inputs(seed: int = 0) -> dict:
    seeds = jax.random.split(jax.random.key(seed), 9)
    return {
        "mixed_qkv": normal_values(seeds[0], (SEQUENCE_TOKENS, 2 * KEY_HEADS * HEAD_DIM + VALUE_HEADS * HEAD_DIM), 1.0, 6.0, ((0, 32),)),
        "gate_z": normal_values(seeds[1], (SEQUENCE_TOKENS, VALUE_HEADS * HEAD_DIM), 1.0, 6.0, ((0, 32),)),
        "gate_logits": draw_gate_logits(jax.random.fold_in(seeds[8], 71), 0),
        "block_table": draw_block_table(jax.random.fold_in(seeds[8], 71), 0),
        "conv_weight": normal_values(seeds[4], (CONV, 2 * KEY_HEADS * HEAD_DIM + VALUE_HEADS * HEAD_DIM), CONV ** -0.5, 3.0, (), jnp.float32),
        "a_log": jnp.clip(jax.random.uniform(seeds[5], (VALUE_HEADS,), jnp.float32, -0.7, 0.7), -0.7, 0.7),
        "dt_bias": jnp.clip(jax.random.uniform(seeds[6], (VALUE_HEADS,), jnp.float32, -0.5, 0.5), -0.5, 0.5),
        "norm_gain": jnp.clip(1.0 + 0.15 * jax.random.normal(seeds[7], (HEAD_DIM,), jnp.float32), 0.25, 1.75),
    }


highest = lax.Precision.HIGHEST

def to_sequence(stored, table):
    columns = stored.shape[1]
    pieces = stored.reshape(N_SEG, 2 * N_CP, TOK_DEV // 2, columns)
    order = jnp.argsort(table, axis=1).astype(jnp.int32)
    picked = jnp.take_along_axis(pieces, order[:, :, None, None], axis=1)
    return picked.reshape(stored.shape[0], columns)

def causal_conv(rows, weights):
    padded = jnp.pad(rows, ((CONV - 1, 0), (0, 0)))
    length = rows.shape[0]
    summed = jnp.zeros(rows.shape, jnp.float32)
    for offset in range(CONV):
        summed = summed + weights[offset] * padded[offset:offset + length].astype(jnp.float32)
    return jax.nn.silu(summed)

def unit_rows(matrix):
    return matrix * lax.rsqrt(lax.optimization_barrier(jnp.sum(matrix * matrix, axis=-1, keepdims=True)) + 1e-06)

def block_terms(queries, key_rows, values, beta_rate, decays):
    cumulative = jnp.cumsum(decays, axis=-1)
    final_sum = cumulative[..., -1:]
    spread = cumulative[..., :, None] - cumulative[..., None, :]
    row_index = lax.broadcasted_iota(jnp.int32, (BLOCK, BLOCK), 0)
    col_index = lax.broadcasted_iota(jnp.int32, (BLOCK, BLOCK), 1)
    strict = row_index > col_index
    inclusive = row_index >= col_index
    strict_decay = jnp.where(strict, jnp.exp(jnp.where(strict, spread, 0.0)), 0.0)
    incl_decay = jnp.where(inclusive, jnp.exp(jnp.where(inclusive, spread, 0.0)), 0.0)
    weighted = key_rows * beta_rate[..., None]
    lower = jnp.einsum('...cd,...ed->...ce', weighted, key_rows, precision=highest) * strict_decay
    system = lower + jnp.eye(BLOCK, dtype=jnp.float32)
    right_side = jnp.concatenate([values * beta_rate[..., None], weighted * jnp.exp(cumulative)[..., None]], axis=-1)
    solved = jax.scipy.linalg.solve_triangular(system, right_side, lower=True, unit_diagonal=True)
    corrected = solved[..., :HEAD_DIM]
    projector = solved[..., HEAD_DIM:]
    key_decay = key_rows * jnp.exp(final_sum - cumulative)[..., None]
    query_decay = queries * jnp.exp(cumulative)[..., None]
    scores = jnp.einsum('...cd,...ed->...ce', queries, key_rows, precision=highest) * incl_decay
    return (corrected, projector, key_decay, query_decay, scores, jnp.exp(final_sum[..., 0]))

def reference(mixed_qkv, gate_z, gate_logits, block_table, conv_weight, a_log, dt_bias, norm_gain):
    seq_qkv = to_sequence(mixed_qkv, block_table)
    seq_z = to_sequence(gate_z, block_table)
    seq_gates = to_sequence(gate_logits, block_table)
    conv_out = causal_conv(seq_qkv, conv_weight)
    length = conv_out.shape[0]
    key_width = KEY_HEADS * HEAD_DIM
    group_size = VALUE_HEADS // KEY_HEADS
    queries = unit_rows(conv_out[:, :key_width].reshape(length, KEY_HEADS, HEAD_DIM)) * HEAD_DIM ** (-0.5)
    key_rows = unit_rows(conv_out[:, key_width:2 * key_width].reshape(length, KEY_HEADS, HEAD_DIM))
    queries = jnp.repeat(queries, group_size, axis=1)
    key_rows = jnp.repeat(key_rows, group_size, axis=1)
    values = conv_out[:, 2 * key_width:].reshape(length, VALUE_HEADS, HEAD_DIM)
    gate_float = seq_gates.astype(jnp.float32)
    beta_rate = jax.nn.sigmoid(gate_float[:, :VALUE_HEADS])
    decays = -jnp.exp(a_log) * jax.nn.softplus(gate_float[:, VALUE_HEADS:] + dt_bias)
    count = length // BLOCK

    def to_blocks(array):
        return array.reshape(count, BLOCK, VALUE_HEADS, HEAD_DIM).transpose(0, 2, 1, 3)

    def to_block_rates(array):
        return array.reshape(count, BLOCK, VALUE_HEADS).transpose(0, 2, 1)

    def block_step(state, pieces):
        query_block, key_block, value_block, beta_block, decay_block = pieces
        corrected, projector, key_decay, query_decay, scores, last_decay = block_terms(query_block, key_block, value_block, beta_block, decay_block)
        new_values = corrected - jnp.einsum('hcd,hde->hce', projector, state, precision=highest)
        outputs = jnp.einsum('hcd,hde->hce', query_decay, state, precision=highest)
        outputs = outputs + jnp.einsum('hce,hev->hcv', scores, new_values, precision=highest)
        state = last_decay[:, None, None] * state + jnp.einsum('hcd,hce->hde', key_decay, new_values, precision=highest)
        return (state, outputs)
    initial = jnp.zeros((VALUE_HEADS, HEAD_DIM, HEAD_DIM), jnp.float32)
    _, blocked = lax.scan(block_step, initial, (to_blocks(queries), to_blocks(key_rows), to_blocks(values), to_block_rates(beta_rate), to_block_rates(decays)))
    core = blocked.transpose(0, 2, 1, 3).reshape(length, VALUE_HEADS, HEAD_DIM)
    gate_values = seq_z.astype(jnp.float32).reshape(length, VALUE_HEADS, HEAD_DIM)
    scale = lax.rsqrt(lax.optimization_barrier(jnp.mean(core * core, axis=-1, keepdims=True)) + 1e-06)
    normed = core * scale * norm_gain * jax.nn.silu(gate_values)
    return normed.reshape(length, VALUE_HEADS * HEAD_DIM).astype(jnp.bfloat16)
```

```python
import functools

import jax
import jax.numpy as jnp
from jax import lax
from jax.experimental import pallas as pl
from jax.experimental.pallas import tpu as pltpu
from jax.sharding import PartitionSpec as P

VALUE_HEADS = 32
KEY_HEADS = 16
HEAD_DIM = 128
CONV = 4
BLOCK = 128
TAIL = 8
GROUP = VALUE_HEADS // KEY_HEADS
BATCH = 4

f32 = jnp.float32
bf16 = jnp.bfloat16
MESH = pl.DeviceIdType.MESH

NN = (((1,), (0,)), ((), ()))
NT = (((1,), (1,)), ((), ()))


def split(x):
    hi = x.astype(bf16)
    return hi, (x - hi.astype(f32)).astype(bf16)


def mm(a, b, dims=NN):
    def dot(x, y):
        return lax.dot_general(x, y, dims, preferred_element_type=f32)

    if dims == NT:
        return dot(a[0], b[0]) + (dot(a[0], b[1]) + dot(a[1], b[0]))
    wide = jnp.concatenate(a, axis=1)
    if b[0].shape[1] > HEAD_DIM:
        return dot(wide, jnp.concatenate([b[0], b[0]], axis=0)) + dot(a[0], b[1])
    top = jnp.concatenate([b[0], b[1]], axis=1)
    low = jnp.concatenate([b[0], jnp.zeros_like(b[1])], axis=1)
    both = dot(wide, jnp.concatenate([top, low], axis=0))
    return both[:, :HEAD_DIM] + both[:, HEAD_DIM:]


def log1p_exact(y):
    u = 1.0 + y
    return jnp.where(u == 1.0, y, jnp.log(u) * (y / jnp.where(u == 1.0, 1.0, u - 1.0)))


def scope(name):
    return jax.named_scope(name)


def squares():
    row = lax.broadcasted_iota(jnp.int32, (BLOCK, BLOCK), 0)
    col = lax.broadcasted_iota(jnp.int32, (BLOCK, BLOCK), 1)
    return row, col


def gate_terms(hpg, half_index, g, row_shift, places, gbuf, rate_ref):
    lane = lax.broadcasted_iota(jnp.int32, (8, BLOCK), 1)
    betas, decays = [], []
    for i0, i1 in places:
        found = []
        for kind in range(2):
            one = pltpu.roll(gbuf[i0, kind].astype(f32), (BLOCK // 2) * half_index, 1)
            two = pltpu.roll(gbuf[i1, kind].astype(f32), (BLOCK // 2) * (1 - half_index), 1)
            found.append(pltpu.roll(jnp.where(lane < BLOCK // 2, one, two), row_shift, 0))
        betas.append(1.0 / (1.0 + jnp.exp(-found[0])))
        shifted = found[1] + rate_ref[g, 1]
        soft = jnp.maximum(shifted, 0.0) + log1p_exact(jnp.exp(-jnp.abs(shifted)))
        decays.append(rate_ref[g, 0] * soft)
    beta = jnp.concatenate(betas, axis=0)
    decay = jnp.concatenate(decays, axis=0)
    row, col = squares()
    upto = jnp.where(row <= col, 1.0, 0.0).astype(bf16)
    d0 = decay.astype(bf16)
    rest = decay - d0.astype(f32)
    d1 = rest.astype(bf16)
    d2 = (rest - d1.astype(f32)).astype(bf16)
    cum = jnp.dot(d2, upto, preferred_element_type=f32)
    cum = cum + jnp.dot(d1, upto, preferred_element_type=f32)
    cum = cum + jnp.dot(d0, upto, preferred_element_type=f32)
    count = beta.shape[0]
    spare = jnp.zeros((BLOCK - 2 * count, BLOCK), f32)
    turned = jnp.transpose(jnp.concatenate([beta, cum, spare], axis=0))
    return cum, turned, count


def prepare(hpg, blk, g, cum, turned, count, w_ref, x_ref):
    row, col = squares()
    strict = row > col
    inclusive = row >= col

    def conv(start):
        cols = slice(start, start + HEAD_DIM)
        total_rows = w_ref[g, 0:1, cols] * x_ref[5 : 5 + BLOCK, cols]
        for j in range(1, CONV):
            total_rows = total_rows + w_ref[g, j : j + 1, cols] * x_ref[5 + j : 5 + j + BLOCK, cols]
        return total_rows / (1.0 + jnp.exp(-total_rows))

    def unit(x):
        return x * lax.rsqrt(jnp.sum(x * x, axis=-1, keepdims=True) + 1e-06)

    queries = unit(conv(0)) * HEAD_DIM ** (-0.5)
    key_rows = unit(conv(HEAD_DIM))
    ks = split(key_rows)
    qs = split(queries)
    kk = mm(ks, ks, NT)
    qk = mm(qs, ks, NT)
    lower, scores, rhs, kdt, qd, last = [], [], [], [], [], []
    for e in range(hpg):
        at = blk * 8 + e
        beta = turned[:, at : at + 1]
        c = turned[:, count + at : count + at + 1]
        ct = cum[at : at + 1, :]
        final = ct[:, BLOCK - 1 :]
        spread = c - ct
        incl = jnp.where(inclusive, jnp.exp(jnp.where(inclusive, spread, 0.0)), 0.0)
        lower.append(jnp.where(strict, beta * kk * incl, 0.0))
        scores.append(split(qk * incl))
        grow = jnp.exp(c)
        values = conv((2 + e) * HEAD_DIM)
        rhs.append(split(jnp.concatenate([values * beta, key_rows * (beta * grow)], axis=1)))
        kdt.append(split(jnp.transpose(key_rows * jnp.exp(final - c))))
        qd.append(queries * grow)
        last.append(jnp.exp(final))
    return lower, scores, rhs, kdt, qd, last


def blocks(n, hpg, g, half_index, first, row_shift, order, cur, prior, gbuf, rate_ref, w_ref, x_ref, o_ref, mh_ref, ml_ref, st_ref):
    half = cur.shape[1]
    row, col = squares()
    eye = jnp.where(row == col, 1.0, 0.0).astype(f32)
    places = [(order[2 * (first + k)], order[2 * (first + k) + 1]) for k in range(BATCH)]
    cum, turned, count = gate_terms(hpg, half_index, g, row_shift, places, gbuf, rate_ref)
    lower, scores, rhs, kdt, qd, last = [], [], [], [], [], []
    for k in range(BATCH):
        b = first + k
        if k:
            x_ref[k, 0:8, :] = cur[places[k - 1][1], half - 16 :, :].astype(f32)[8:]
        else:
            ahead = order[jnp.maximum(2 * b - 1, 0)]
            near = cur[ahead, half - 16 :, :].astype(f32)[8:]
            x_ref[k, 0:8, :] = jnp.where(lax.rem(b, n // 2) == 0, prior[...], near)
        x_ref[k, 8 : 8 + half, :] = cur[places[k][0]].astype(f32)
        x_ref[k, 8 + half : 8 + 2 * half, :] = cur[places[k][1]].astype(f32)
        found = prepare(hpg, k, g, cum, turned, count, w_ref, x_ref.at[k])
        for total, more in zip((lower, scores, rhs, kdt, qd, last), found):
            total += more
    hs = range(BATCH * hpg)

    def same(size):
        return (row // size) == (col // size)

    small = 16
    power = [split(jnp.where(same(small), -lower[h], 0.0)) for h in hs]
    inverse = [eye + jnp.where(same(small), -lower[h], 0.0) for h in hs]
    steps = 1
    while 2**steps < small:
        power = [split(mm(power[h], power[h])) for h in hs]
        inverse = [inverse[h] + mm(split(inverse[h]), power[h]) for h in hs]
        steps += 1
    size = small
    while size < BLOCK:
        between = same(2 * size) & (~same(size))
        cross = [split(jnp.where(between, lower[h], 0.0)) for h in hs]
        parts = [split(inverse[h]) for h in hs]
        mixed = [split(mm(cross[h], parts[h])) for h in hs]
        inverse = [inverse[h] - mm(parts[h], mixed[h]) for h in hs]
        size *= 2
    solved = [split(mm(split(inverse[h]), rhs[h])) for h in hs]
    outs = [mm(scores[h], solved[h]) for h in hs]
    ends = [mm(kdt[h], solved[h]) for h in hs]
    readers = [split(qd[h] - outs[h][:, HEAD_DIM:]) for h in hs]
    maps = [split(last[h] * eye - ends[h][:, HEAD_DIM:]) for h in hs]
    for k in range(BATCH):
        b = first + k
        states = [split(st_ref[g, e]) for e in range(hpg)]
        for e in range(hpg):
            at = k * hpg + e
            moved = mm(maps[at], states[e])
            st_ref[g, e] = jnp.concatenate(
                [moved[:, :HEAD_DIM] + ends[at][:, :HEAD_DIM], moved[:, HEAD_DIM:]], axis=1
            )
        for e in range(hpg):
            at = k * hpg + e
            seen = mm(readers[at], states[e])
            o_ref[g * hpg + e, b] = seen[:, :HEAD_DIM] + outs[at][:, :HEAD_DIM]
            reach = split(seen[:, HEAD_DIM:])
            mh_ref[g * hpg + e, b] = reach[0]
            ml_ref[g * hpg + e, b] = reach[1]


def whole_kernel(
    n, segs, heads, table, a_log, dt_bias, table_any, qkv, z, gates, conv_weight, gain_ref, out,
    xin, otail, gbuf, ptab, cur, prior, x_ref, w_ref, rate_ref, order, o_ref, mh_ref, ml_ref, st_ref,
    inc_ref, pass_ref, y_ref, local, lout, ssem, rsem, hsend, hrecv, *oz
):
    me = lax.axis_index("cp")
    seg = lax.axis_index("seg")
    final = segs - 1
    after = lax.rem(seg + 1, segs)
    before = lax.rem(seg + segs - 1, segs)
    keys = max(1, heads // GROUP)
    hpg = heads // keys
    units = 2 * keys
    key_width = KEY_HEADS * HEAD_DIM
    width = heads * HEAD_DIM
    wz = hpg * HEAD_DIM
    rows = qkv.shape[0]
    half = rows // 2
    AT_TAIL, AT_GATE, AT_Z, AT_TABLE, AT_Y = units, units + keys, units + keys + 1, units + 2 * keys + 1, units + 2 * keys + 2

    barrier = pltpu.get_barrier_semaphore()
    for d in range(1, n):
        pl.semaphore_signal(barrier, inc=1, device_id=(seg, lax.rem(me + d, n)), device_id_type=MESH)

    @pl.when(seg > 0)
    def _():
        for d in range(n):
            pl.semaphore_signal(barrier, inc=1, device_id=(before, lax.rem(me + d, n)), device_id_type=MESH)

    def columns(start, size):
        return pl.ds(pl.multiple_of(start, HEAD_DIM), size)

    def places(p, g):
        key = (lax.div(p * heads, GROUP) + g) * HEAD_DIM
        value = (p * heads + g * hpg) * HEAD_DIM
        return (
            (columns(key, HEAD_DIM), pl.ds(0, HEAD_DIM)),
            (columns(key_width + key, HEAD_DIM), pl.ds(HEAD_DIM, HEAD_DIM)),
            (columns(2 * key_width + value, wz), pl.ds(2 * HEAD_DIM, wz)),
        )

    def unit_pieces(p, u, slot):
        these = pl.ds((u % 2) * half, half)
        return [(qkv.at[these, src], xin.at[u, slot, :, dst]) for src, dst in places(p, u // 2)]

    def tail_pieces(p, g, slot):
        these = pl.ds(rows - TAIL, TAIL)
        return [(qkv.at[these, src], otail.at[g, slot, :, dst]) for src, dst in places(p, g)]

    def gate_pieces(p, slot):
        tile = lax.div(p * heads, 8) * 8
        return [
            (gates.at[pl.ds(pl.multiple_of(kind * VALUE_HEADS + tile, 8), 8)], gbuf.at[slot, kind]) for kind in range(2)
        ]

    def z_pieces(p, g, slot):
        cols = columns((p * heads + g * hpg) * HEAD_DIM, wz)
        return [(z.at[pl.ds(hf * half, half), cols], oz[g].at[slot, hf]) for hf in range(2)]

    for g in range(keys):
        for src, dst in places(me, g):
            pltpu.make_async_copy(conv_weight.at[:, src], w_ref.at[g, :, dst], lout.at[0]).start()
    for kind, found in enumerate(
        [unit_pieces(me, u, me) for u in range(units)]
        + [gate_pieces(me, me)]
        + [z_pieces(me, g, me) for g in range(keys)]
    ):
        for src, dst in found:
            pltpu.make_async_copy(src, dst, local.at[kind]).start()
    with scope("entry"):
        pl.semaphore_wait(barrier, n - 1 + jnp.where(seg < final, n, 0))

    def post(kind, src, dst, target):
        pltpu.make_async_remote_copy(
            src_ref=src, dst_ref=dst, send_sem=ssem.at[kind], recv_sem=rsem.at[kind],
            device_id=target, device_id_type=MESH,
        ).start()

    def remote(kind, ref):
        return pltpu.make_async_remote_copy(
            src_ref=ref, dst_ref=ref, send_sem=ssem.at[kind], recv_sem=rsem.at[kind],
            device_id=(seg, lax.rem(me + 1, n)), device_id_type=MESH,
        )

    others = pl.ds(0, n - 1)

    def post_tails(g):
        @pl.when(seg < final)
        def _():
            if g == 0:
                post(AT_TABLE, table_any, ptab, (after, me))
            for d in range(n):
                peer = lax.rem(me + d, n)
                for src, dst in tail_pieces(peer, g, me):
                    post(AT_TAIL + g, src, dst, (after, peer))

    def post_all(kind, find):
        for d in range(1, n):
            peer = lax.rem(me + d, n)
            for src, dst in find(peer):
                post(kind, src, dst, (seg, peer))

    post_all(AT_GATE, lambda p: gate_pieces(p, me))
    for g in range(keys):
        post_tails(g)
        for u in (2 * g, 2 * g + 1):
            post_all(u, lambda p: unit_pieces(p, u, me))
    for g in range(keys):
        post_all(AT_Z + g, lambda p: z_pieces(p, g, me))

    def find(b, carry):
        parity = lax.div(b, n)
        place = jnp.int32(0)
        for j in range(n):
            place = jnp.where(table[0, 2 * j + parity] == b, j, place)
        order[b] = place
        return carry

    lax.fori_loop(0, 2 * n, find, 0)

    row, col = squares()
    line = lax.broadcasted_iota(jnp.int32, (8, BLOCK), 0)
    for g in range(keys):
        scale = jnp.zeros((8, BLOCK), f32)
        shift = jnp.zeros((8, BLOCK), f32)
        for e in range(hpg):
            h = me * heads + g * hpg + e
            scale = jnp.where(line == e, a_log[h], scale)
            shift = jnp.where(line == e, dt_bias[h], shift)
            st_ref[g, e, :, :HEAD_DIM] = jnp.zeros((HEAD_DIM, HEAD_DIM), f32)
            st_ref[g, e, :, HEAD_DIM:] = jnp.where(row == col, 1.0, 0.0).astype(f32)
        rate_ref[g, 0] = -jnp.exp(scale)
        rate_ref[g, 1] = shift

    pltpu.make_async_copy(w_ref, w_ref, lout.at[0]).wait()
    pltpu.make_async_copy(gbuf.at[me], gbuf.at[me], local.at[units]).wait()
    with scope("gatewait"):
        remote(AT_GATE, gbuf.at[others]).wait_recv()

    @pl.when(seg > 0)
    def _():
        remote(AT_TABLE, ptab).wait_recv()

    def hop(h):
        return pltpu.make_async_remote_copy(
            src_ref=pass_ref.at[h],
            dst_ref=inc_ref.at[h],
            send_sem=hsend.at[h],
            recv_sem=hrecv.at[h],
            device_id=(after, me),
            device_id_type=MESH,
        )

    def forward(g):
        @pl.when(seg == 0)
        def _():
            for e in range(hpg):
                h = g * hpg + e
                pass_ref[h] = st_ref[g, e, :, :HEAD_DIM]
                hop(h).start()

        @pl.when((seg > 0) & (seg < final))
        def _():
            for e in range(hpg):
                h = g * hpg + e
                through = split(st_ref[g, e, :, HEAD_DIM:])
                with scope("hopmid"):
                    hop(h).wait_recv()
                pass_ref[h] = st_ref[g, e, :, :HEAD_DIM] + mm(through, split(inc_ref[h]))
                hop(h).start()

    def one_unit(u, carry):
        g = lax.div(u, 2)
        half_index = lax.rem(u, 2)
        with scope("unitwait"):
            pltpu.make_async_copy(xin.at[u, me], xin.at[u, me], local.at[u]).wait()
            remote(u, xin.at[u, others]).wait_recv()

        @pl.when((half_index == 0) & (seg == 0))
        def _():
            prior[...] = jnp.zeros_like(prior)

        @pl.when((half_index == 0) & (seg > 0))
        def _():
            with scope("tailwait"):
                remote(AT_TAIL + g, otail.at[g]).wait_recv()
            found = jnp.zeros(prior.shape, f32)
            for j in range(n):
                hit = ptab[0:1, 2 * j + 1 : 2 * j + 2] == 2 * n - 1
                found = jnp.where(hit, otail[g, j].astype(f32), found)
            prior[...] = found

        @pl.when(half_index == 1)
        def _():
            prior[...] = cur[order[n - 1], half - 16 :, :].astype(f32)[8:]

        cur[...] = xin[u]
        row_shift = lax.rem(8 - lax.rem(me * heads, 8) - g * hpg + 8, 8)

        def batch(first):
            blocks(
                n, hpg, g, half_index, first, row_shift, order, cur, prior, gbuf, rate_ref,
                w_ref, x_ref, o_ref, mh_ref, ml_ref, st_ref,
            )

        turns = n // 2 // BATCH
        with scope("run"):
            if turns == 1:
                batch(half_index * (n // 2))
            else:
                lax.fori_loop(0, turns, lambda t, c: (batch(half_index * (n // 2) + t * BATCH), c)[1], 0)
        for earlier in range(keys - 1):
            @pl.when(u == jnp.minimum(2 * earlier + 1 + seg, units - 1))
            def _():
                forward(earlier)
        return carry

    lax.fori_loop(0, units, one_unit, 0)

    def block(h, b, state):
        g, e = h // hpg, h % hpg
        i0 = order[2 * b]
        i1 = order[2 * b + 1]
        which = lax.div(b, n // 2)
        cols = pl.ds(e * HEAD_DIM, HEAD_DIM)
        core = o_ref[h, b] + mm((mh_ref[h, b], ml_ref[h, b]), state)
        gate = jnp.concatenate([oz[g][i0, which, :, cols], oz[g][i1, which, :, cols]], axis=0).astype(f32)
        scale = lax.rsqrt(jnp.sum(core * core, axis=-1, keepdims=True) * (1.0 / HEAD_DIM) + 1e-06)
        y_ref[h, b] = (core * scale * gain_ref[0:1, :] * (gate / (1.0 + jnp.exp(-gate)))).astype(bf16)

    def target(h, source):
        return out.at[:, columns(source * width + h * HEAD_DIM, HEAD_DIM)]

    def give(h, d):
        peer = lax.rem(me + d, n)
        post(AT_Y, y_ref.at[h, peer], target(h, me), (seg, peer))

    def close(h):
        @pl.when(seg == 0)
        def _():
            inc_ref[h] = jnp.zeros((HEAD_DIM, HEAD_DIM), f32)

        @pl.when(seg == final)
        def _():
            with scope("hoplast"):
                hop(h).wait_recv()

        state = split(inc_ref[h])
        for d in range(1, n):
            block(h, lax.rem(me + d, n), state)
            if d > 1:
                give(h, d - 1)
        block(h, me, state)
        give(h, n - 1)
        pltpu.make_async_copy(y_ref.at[h, me], target(h, me), lout.at[1]).start()

    for h in range(heads):
        g = h // hpg
        if h % hpg == 0:
            for kind in (AT_Z + g,):
                pltpu.make_async_copy(oz[g].at[me], oz[g].at[me], local.at[units + 1 + g]).wait()
                with scope("zwait"):
                    remote(kind, oz[g].at[others]).wait_recv()
        if h == min(hpg, heads - hpg):
            with scope("forward_late"):
                pl.when(seg > 1)(lambda: forward(keys - 1))
        if h == 0:
            with scope("forward_early"):
                pl.when(seg <= 1)(lambda: forward(keys - 1))
        with scope("close"):
            close(h)

    with scope("waity"):
        pltpu.make_async_copy(y_ref.at[:, 0], y_ref.at[:, 0], lout.at[1]).wait()
        remote(AT_Y, y_ref.at[:, others]).wait_recv()
    with scope("drain"):
        remote(AT_GATE, gbuf.at[others]).wait_send()
        for u in range(units):
            remote(u, xin.at[u, others]).wait_send()
        for g in range(keys):
            remote(AT_Z + g, oz[g].at[others]).wait_send()
        remote(AT_Y, y_ref.at[:, others]).wait_send()

        @pl.when(seg < final)
        def _():
            remote(AT_TABLE, ptab).wait_send()
            for g in range(keys):
                remote(AT_TAIL + g, otail.at[g]).wait_send()
            for h in range(heads):
                hop(h).wait_send()


def mixer(n, segs, heads, table, a_log, dt_bias, qkv, z, gates, conv_weight, gain):
    keys = max(1, heads // GROUP)
    hpg = heads // keys
    units = 2 * keys
    half = qkv.shape[0] // 2
    wide = (2 + hpg) * HEAD_DIM
    anywhere = pl.BlockSpec(memory_space=pl.ANY)
    vmem = pl.BlockSpec(memory_space=pltpu.VMEM)
    smem = pl.BlockSpec(memory_space=pltpu.SMEM)
    square = (HEAD_DIM, HEAD_DIM)
    DMA = pltpu.SemaphoreType.DMA
    kinds = units + 2 * keys + 3
    return pl.pallas_call(
        functools.partial(whole_kernel, n, segs, heads),
        out_shape=pltpu.VMEM((BLOCK, n * heads * HEAD_DIM), bf16),
        in_specs=[smem] * 3 + [anywhere] * 5 + [vmem],
        out_specs=vmem,
        scratch_shapes=[
            pltpu.VMEM((units, n, half, wide), bf16),
            pltpu.VMEM((keys, n, TAIL, wide), bf16),
            pltpu.VMEM((n, 2, 8, BLOCK), bf16),
            pltpu.VMEM(table.shape, jnp.int32),
            pltpu.VMEM((n, half, wide), bf16),
            pltpu.VMEM((TAIL, wide), f32),
            pltpu.VMEM((BATCH, BLOCK + 8, wide), f32),
            pltpu.VMEM((keys, CONV, wide), f32),
            pltpu.VMEM((keys, 2, 8, BLOCK), f32),
            pltpu.SMEM((2 * n,), jnp.int32),
            pltpu.VMEM((heads, n) + square, f32),
            pltpu.VMEM((heads, n) + square, bf16),
            pltpu.VMEM((heads, n) + square, bf16),
            pltpu.VMEM((keys, hpg, HEAD_DIM, 2 * HEAD_DIM), f32),
            pltpu.VMEM((heads,) + square, f32),
            pltpu.VMEM((heads,) + square, f32),
            pltpu.VMEM((heads, n) + square, bf16),
            DMA((units + 1 + keys,)),
            DMA((2,)),
            DMA((kinds,)),
            DMA((kinds,)),
            DMA((heads,)),
            DMA((heads,)),
        ]
        + [pltpu.VMEM((n, 2, half, hpg * HEAD_DIM), bf16)] * keys,
        compiler_params=pltpu.CompilerParams(
            collective_id=0, has_side_effects=True, vmem_limit_bytes=48 * 1024 * 1024
        ),
        name="mixer",
    )(*[pltpu.with_memory_space_constraint(x, pltpu.HBM) for x in (table, a_log, dt_bias, table, qkv, z, gates, conv_weight, gain)])


def per_device(mixed_qkv, gate_z, gate_logits, block_table, conv_weight, a_log, dt_bias, norm_gain):
    n = lax.axis_size("cp")
    segs = lax.axis_size("seg")
    return mixer(
        n, segs, VALUE_HEADS // n, block_table, a_log, dt_bias, mixed_qkv, gate_z, gate_logits.T,
        conv_weight, norm_gain[None, :],
    )


def solution(mesh):
    return jax.shard_map(
        per_device,
        mesh=mesh,
        in_specs=(
            P(("seg", "cp"), None),
            P(("seg", "cp"), None),
            P(("seg", "cp"), None),
            P("seg", None),
            P(),
            P(),
            P(),
            P(),
        ),
        out_specs=P(("seg", "cp"), None),
        check_vma=False,
    )
```

```python
import functools

import jax
import jax.numpy as jnp
from jax import lax
from jax.experimental import pallas as pl
from jax.experimental.pallas import tpu as pltpu
from jax.sharding import PartitionSpec as P

VALUE_HEADS = 32
KEY_HEADS = 16
HEAD_DIM = 128
CONV = 4
BLOCK = 128
TAIL = 8
GROUP = VALUE_HEADS // KEY_HEADS
BATCH = 4

f32 = jnp.float32
bf16 = jnp.bfloat16
MESH = pl.DeviceIdType.MESH

NN = (((1,), (0,)), ((), ()))
NT = (((1,), (1,)), ((), ()))


def split(x):
    hi = x.astype(bf16)
    return hi, (x - hi.astype(f32)).astype(bf16)


def mm(a, b, dims=NN):
    def dot(x, y):
        return lax.dot_general(x, y, dims, preferred_element_type=f32)

    if dims == NT:
        return dot(a[0], b[0]) + (dot(a[0], b[1]) + dot(a[1], b[0]))
    wide = jnp.concatenate(a, axis=1)
    if b[0].shape[1] > HEAD_DIM:
        return dot(wide, jnp.concatenate([b[0], b[0]], axis=0)) + dot(a[0], b[1])
    top = jnp.concatenate([b[0], b[1]], axis=1)
    low = jnp.concatenate([b[0], jnp.zeros_like(b[1])], axis=1)
    both = dot(wide, jnp.concatenate([top, low], axis=0))
    return both[:, :HEAD_DIM] + both[:, HEAD_DIM:]


def log1p_exact(y):
    u = 1.0 + y
    return jnp.where(u == 1.0, y, jnp.log(u) * (y / jnp.where(u == 1.0, 1.0, u - 1.0)))


def scope(name):
    return jax.named_scope(name)


def squares():
    row = lax.broadcasted_iota(jnp.int32, (BLOCK, BLOCK), 0)
    col = lax.broadcasted_iota(jnp.int32, (BLOCK, BLOCK), 1)
    return row, col


def gate_terms(hpg, half_index, g, row_shift, places, gbuf, rate_ref):
    lane = lax.broadcasted_iota(jnp.int32, (8, BLOCK), 1)
    betas, decays = [], []
    for i0, i1 in places:
        found = []
        for kind in range(2):
            one = pltpu.roll(gbuf[i0, kind].astype(f32), (BLOCK // 2) * half_index, 1)
            two = pltpu.roll(gbuf[i1, kind].astype(f32), (BLOCK // 2) * (1 - half_index), 1)
            found.append(pltpu.roll(jnp.where(lane < BLOCK // 2, one, two), row_shift, 0))
        betas.append(1.0 / (1.0 + jnp.exp(-found[0])))
        shifted = found[1] + rate_ref[g, 1]
        soft = jnp.maximum(shifted, 0.0) + log1p_exact(jnp.exp(-jnp.abs(shifted)))
        decays.append(rate_ref[g, 0] * soft)
    beta = jnp.concatenate(betas, axis=0)
    decay = jnp.concatenate(decays, axis=0)
    row, col = squares()
    upto = jnp.where(row <= col, 1.0, 0.0).astype(bf16)
    d0 = decay.astype(bf16)
    rest = decay - d0.astype(f32)
    d1 = rest.astype(bf16)
    d2 = (rest - d1.astype(f32)).astype(bf16)
    cum = jnp.dot(d2, upto, preferred_element_type=f32)
    cum = cum + jnp.dot(d1, upto, preferred_element_type=f32)
    cum = cum + jnp.dot(d0, upto, preferred_element_type=f32)
    count = beta.shape[0]
    spare = jnp.zeros((BLOCK - 2 * count, BLOCK), f32)
    turned = jnp.transpose(jnp.concatenate([beta, cum, spare], axis=0))
    return cum, turned, count


def prepare(hpg, blk, g, cum, turned, count, w_ref, x_ref):
    row, col = squares()
    strict = row > col
    inclusive = row >= col

    def conv(start):
        cols = slice(start, start + HEAD_DIM)
        total_rows = w_ref[g, 0:1, cols] * x_ref[5 : 5 + BLOCK, cols]
        for j in range(1, CONV):
            total_rows = total_rows + w_ref[g, j : j + 1, cols] * x_ref[5 + j : 5 + j + BLOCK, cols]
        return total_rows / (1.0 + jnp.exp(-total_rows))

    def unit(x):
        return x * lax.rsqrt(jnp.sum(x * x, axis=-1, keepdims=True) + 1e-06)

    queries = unit(conv(0)) * HEAD_DIM ** (-0.5)
    key_rows = unit(conv(HEAD_DIM))
    ks = split(key_rows)
    qs = split(queries)
    kk = mm(ks, ks, NT)
    qk = mm(qs, ks, NT)
    lower, scores, rhs, kdt, qd, last = [], [], [], [], [], []
    for e in range(hpg):
        at = blk * 8 + e
        beta = turned[:, at : at + 1]
        c = turned[:, count + at : count + at + 1]
        ct = cum[at : at + 1, :]
        final = ct[:, BLOCK - 1 :]
        spread = c - ct
        incl = jnp.where(inclusive, jnp.exp(jnp.where(inclusive, spread, 0.0)), 0.0)
        lower.append(jnp.where(strict, beta * kk * incl, 0.0))
        scores.append(split(qk * incl))
        grow = jnp.exp(c)
        values = conv((2 + e) * HEAD_DIM)
        rhs.append(split(jnp.concatenate([values * beta, key_rows * (beta * grow)], axis=1)))
        kdt.append(split(jnp.transpose(key_rows * jnp.exp(final - c))))
        qd.append(queries * grow)
        last.append(jnp.exp(final))
    return lower, scores, rhs, kdt, qd, last


def blocks(n, hpg, g, half_index, first, row_shift, order, cur, prior, gbuf, rate_ref, w_ref, x_ref, o_ref, mh_ref, ml_ref, st_ref):
    half = cur.shape[1]
    row, col = squares()
    eye = jnp.where(row == col, 1.0, 0.0).astype(f32)
    places = [(order[2 * (first + k)], order[2 * (first + k) + 1]) for k in range(BATCH)]
    cum, turned, count = gate_terms(hpg, half_index, g, row_shift, places, gbuf, rate_ref)
    lower, scores, rhs, kdt, qd, last = [], [], [], [], [], []
    for k in range(BATCH):
        b = first + k
        if k:
            x_ref[k, 0:8, :] = cur[places[k - 1][1], half - 16 :, :].astype(f32)[8:]
        else:
            ahead = order[jnp.maximum(2 * b - 1, 0)]
            near = cur[ahead, half - 16 :, :].astype(f32)[8:]
            x_ref[k, 0:8, :] = jnp.where(lax.rem(b, n // 2) == 0, prior[...], near)
        x_ref[k, 8 : 8 + half, :] = cur[places[k][0]].astype(f32)
        x_ref[k, 8 + half : 8 + 2 * half, :] = cur[places[k][1]].astype(f32)
        found = prepare(hpg, k, g, cum, turned, count, w_ref, x_ref.at[k])
        for total, more in zip((lower, scores, rhs, kdt, qd, last), found):
            total += more
    hs = range(BATCH * hpg)

    def same(size):
        return (row // size) == (col // size)

    small = 16
    power = [split(jnp.where(same(small), -lower[h], 0.0)) for h in hs]
    inverse = [eye + jnp.where(same(small), -lower[h], 0.0) for h in hs]
    steps = 1
    while 2**steps < small:
        power = [split(mm(power[h], power[h])) for h in hs]
        inverse = [inverse[h] + mm(split(inverse[h]), power[h]) for h in hs]
        steps += 1
    size = small
    while size < BLOCK:
        between = same(2 * size) & (~same(size))
        cross = [split(jnp.where(between, lower[h], 0.0)) for h in hs]
        parts = [split(inverse[h]) for h in hs]
        mixed = [split(mm(cross[h], parts[h])) for h in hs]
        inverse = [inverse[h] - mm(parts[h], mixed[h]) for h in hs]
        size *= 2
    solved = [split(mm(split(inverse[h]), rhs[h])) for h in hs]
    outs = [mm(scores[h], solved[h]) for h in hs]
    ends = [mm(kdt[h], solved[h]) for h in hs]
    readers = [split(qd[h] - outs[h][:, HEAD_DIM:]) for h in hs]
    maps = [split(last[h] * eye - ends[h][:, HEAD_DIM:]) for h in hs]
    for k in range(BATCH):
        b = first + k
        states = [split(st_ref[g, e]) for e in range(hpg)]
        for e in range(hpg):
            at = k * hpg + e
            moved = mm(maps[at], states[e])
            st_ref[g, e] = jnp.concatenate(
                [moved[:, :HEAD_DIM] + ends[at][:, :HEAD_DIM], moved[:, HEAD_DIM:]], axis=1
            )
        for e in range(hpg):
            at = k * hpg + e
            seen = mm(readers[at], states[e])
            o_ref[g * hpg + e, b] = seen[:, :HEAD_DIM] + outs[at][:, :HEAD_DIM]
            reach = split(seen[:, HEAD_DIM:])
            mh_ref[g * hpg + e, b] = reach[0]
            ml_ref[g * hpg + e, b] = reach[1]


def whole_kernel(
    n, segs, heads, table_any, a_log_any, dt_bias_any, qkv, z, gates, conv_weight, gain_any, out,
    table, a_log, dt_bias, gain_ref, stage, gstage, tstage, tsend,
    xin, otail, gbuf, ptab, cur, prior, x_ref, w_ref, rate_ref, order, o_ref, mh_ref, ml_ref, st_ref,
    inc_ref, pass_ref, y_ref, lin, local, lout, ssem, rsem, hsend, hrecv, ready, *oz
):
    me = lax.axis_index("cp")
    seg = lax.axis_index("seg")
    final = segs - 1
    after = lax.rem(seg + 1, segs)
    before = lax.rem(seg + segs - 1, segs)
    keys = max(1, heads // GROUP)
    hpg = heads // keys
    units = 2 * keys
    key_width = KEY_HEADS * HEAD_DIM
    width = heads * HEAD_DIM
    wz = hpg * HEAD_DIM
    rows = qkv.shape[0]
    half = rows // 2
    AT_TAIL, AT_GATE, AT_Z, AT_TABLE, AT_Y = units, units + keys, units + keys + 1, units + 2 * keys + 1, units + 2 * keys + 2

    barrier = pltpu.get_barrier_semaphore()
    for d in range(1, n):
        pl.semaphore_signal(barrier, inc=1, device_id=(seg, lax.rem(me + d, n)), device_id_type=MESH)

    @pl.when(seg < final)
    def _():
        pl.semaphore_signal(barrier, inc=1, device_id=(after, me), device_id_type=MESH)

    small = [
        pltpu.make_async_copy(src, dst, lin.at[i])
        for i, (src, dst) in enumerate(
            (
                (qkv.at[pl.ds(0, half)], stage),
                (gates, gstage),
                (qkv.at[pl.ds(rows - TAIL, TAIL)], tstage),
                (table_any, table),
                (a_log_any, a_log),
                (dt_bias_any, dt_bias),
                (gain_any, gain_ref),
            )
        )
    ]
    for copy in small:
        copy.start()

    def columns(start, size):
        return pl.ds(pl.multiple_of(start, HEAD_DIM), size)

    def places(p, g):
        key = (lax.div(p * heads, GROUP) + g) * HEAD_DIM
        value = (p * heads + g * hpg) * HEAD_DIM
        return (
            (columns(key, HEAD_DIM), pl.ds(0, HEAD_DIM)),
            (columns(key_width + key, HEAD_DIM), pl.ds(HEAD_DIM, HEAD_DIM)),
            (columns(2 * key_width + value, wz), pl.ds(2 * HEAD_DIM, wz)),
        )

    def unit_pieces(p, u, slot):
        if u % 2 == 0:
            return [(stage.at[:, src], xin.at[u, slot, :, dst]) for src, dst in places(p, u // 2)]
        return [(qkv.at[pl.ds(half, half), src], xin.at[u, slot, :, dst]) for src, dst in places(p, u // 2)]

    def gate_pieces(p, slot):
        tile = lax.div(p * heads, 8) * 8
        return [
            (gstage.at[pl.ds(pl.multiple_of(kind * VALUE_HEADS + tile, 8), 8)], gbuf.at[slot, kind]) for kind in range(2)
        ]

    def z_pieces(p, g, slot):
        cols = columns((p * heads + g * hpg) * HEAD_DIM, wz)
        return [(z.at[pl.ds(hf * half, half), cols], oz[g].at[slot, hf]) for hf in range(2)]

    for g in range(keys):
        for src, dst in places(me, g):
            pltpu.make_async_copy(conv_weight.at[:, src], w_ref.at[g, :, dst], lout.at[0]).start()
    small[0].wait()
    small[1].wait()
    for kind, found in enumerate(
        [unit_pieces(me, u, me) for u in range(units)]
        + [gate_pieces(me, me)]
        + [z_pieces(me, g, me) for g in range(keys)]
    ):
        for src, dst in found:
            pltpu.make_async_copy(src, dst, local.at[kind]).start()
    with scope("entry"):
        pl.semaphore_wait(barrier, n - 1 + jnp.where(seg > 0, 1, 0))

    @pl.when(seg > 0)
    def _():
        pl.semaphore_signal(ready, inc=1, device_id=(before, me), device_id_type=MESH)

    def post(kind, src, dst, target):
        pltpu.make_async_remote_copy(
            src_ref=src, dst_ref=dst, send_sem=ssem.at[kind], recv_sem=rsem.at[kind],
            device_id=target, device_id_type=MESH,
        ).start()

    def remote(kind, ref):
        return pltpu.make_async_remote_copy(
            src_ref=ref, dst_ref=ref, send_sem=ssem.at[kind], recv_sem=rsem.at[kind],
            device_id=(seg, lax.rem(me + 1, n)), device_id_type=MESH,
        )

    others = pl.ds(0, n - 1)

    def post_all(kind, find):
        for d in range(1, n):
            peer = lax.rem(me + d, n)
            for src, dst in find(peer):
                post(kind, src, dst, (seg, peer))

    post_all(AT_GATE, lambda p: gate_pieces(p, me))
    post_all(0, lambda p: unit_pieces(p, 0, me))
    for copy in small[2:]:
        copy.wait()

    wide = hpg + 2
    pairs = (wide + 1) // 2
    upper = lax.broadcasted_iota(jnp.int32, (TAIL, HEAD_DIM), 0) < TAIL // 2
    for g in range(keys):
        for p in range(n):
            key = p * heads // GROUP + g
            at = [key, KEY_HEADS + key] + [2 * KEY_HEADS + p * heads + g * hpg + e for e in range(hpg)]
            tiles = [tstage[:, i * HEAD_DIM : (i + 1) * HEAD_DIM].astype(f32) for i in at]
            for i in range(pairs):
                low = tiles[i + pairs] if i + pairs < wide else tiles[i]
                both = jnp.where(upper, pltpu.roll(tiles[i], TAIL // 2, 0), low)
                tsend[g, p, :, i * HEAD_DIM : (i + 1) * HEAD_DIM] = both.astype(bf16)

    @pl.when(seg < final)
    def _():
        with scope("readywait"):
            pl.semaphore_wait(ready, 1)
        post(AT_TABLE, table_any, ptab, (after, me))
        for g in range(keys):
            for d in range(n):
                peer = lax.rem(me + d, n)
                post(AT_TAIL + g, tsend.at[g, peer], otail.at[g, me], (after, peer))

    for u in range(1, units):
        post_all(u, lambda p: unit_pieces(p, u, me))
    for g in range(keys):
        post_all(AT_Z + g, lambda p: z_pieces(p, g, me))

    def find(b, carry):
        parity = lax.div(b, n)
        place = jnp.int32(0)
        for j in range(n):
            place = jnp.where(table[0, 2 * j + parity] == b, j, place)
        order[b] = place
        return carry

    lax.fori_loop(0, 2 * n, find, 0)

    row, col = squares()
    line = lax.broadcasted_iota(jnp.int32, (8, BLOCK), 0)
    for g in range(keys):
        scale = jnp.zeros((8, BLOCK), f32)
        shift = jnp.zeros((8, BLOCK), f32)
        for e in range(hpg):
            h = me * heads + g * hpg + e
            scale = jnp.where(line == e, a_log[h], scale)
            shift = jnp.where(line == e, dt_bias[h], shift)
            st_ref[g, e, :, :HEAD_DIM] = jnp.zeros((HEAD_DIM, HEAD_DIM), f32)
            st_ref[g, e, :, HEAD_DIM:] = jnp.where(row == col, 1.0, 0.0).astype(f32)
        rate_ref[g, 0] = -jnp.exp(scale)
        rate_ref[g, 1] = shift

    pltpu.make_async_copy(w_ref, w_ref, lout.at[0]).wait()
    pltpu.make_async_copy(gbuf.at[me], gbuf.at[me], local.at[units]).wait()
    with scope("gatewait"):
        remote(AT_GATE, gbuf.at[others]).wait_recv()

    @pl.when(seg > 0)
    def _():
        remote(AT_TABLE, ptab).wait_recv()

    def hop(h):
        return pltpu.make_async_remote_copy(
            src_ref=pass_ref.at[h],
            dst_ref=inc_ref.at[h],
            send_sem=hsend.at[h],
            recv_sem=hrecv.at[h],
            device_id=(after, me),
            device_id_type=MESH,
        )

    def forward(g):
        @pl.when(seg == 0)
        def _():
            for e in range(hpg):
                h = g * hpg + e
                pass_ref[h] = st_ref[g, e, :, :HEAD_DIM]
                hop(h).start()

        @pl.when((seg > 0) & (seg < final))
        def _():
            for e in range(hpg):
                h = g * hpg + e
                through = split(st_ref[g, e, :, HEAD_DIM:])
                with scope("hopmid"):
                    hop(h).wait_recv()
                pass_ref[h] = st_ref[g, e, :, :HEAD_DIM] + mm(through, split(inc_ref[h]))
                hop(h).start()

    def one_unit(u, carry):
        g = lax.div(u, 2)
        half_index = lax.rem(u, 2)
        with scope("unitwait"):
            pltpu.make_async_copy(xin.at[u, me], xin.at[u, me], local.at[u]).wait()
            remote(u, xin.at[u, others]).wait_recv()

        @pl.when((half_index == 0) & (seg == 0))
        def _():
            prior[...] = jnp.zeros_like(prior)

        @pl.when((half_index == 0) & (seg > 0))
        def _():
            with scope("tailwait"):
                remote(AT_TAIL + g, otail.at[g]).wait_recv()
            found = jnp.zeros(otail.shape[2:], f32)
            for j in range(n):
                hit = ptab[0:1, 2 * j + 1 : 2 * j + 2] == 2 * n - 1
                found = jnp.where(hit, otail[g, j].astype(f32), found)
            for i in range(wide):
                pair = found[:, i % pairs * HEAD_DIM : (i % pairs + 1) * HEAD_DIM]
                prior[:, i * HEAD_DIM : (i + 1) * HEAD_DIM] = pltpu.roll(pair, TAIL // 2, 0) if i < pairs else pair

        @pl.when(half_index == 1)
        def _():
            prior[...] = cur[order[n - 1], half - 16 :, :].astype(f32)[8:]

        cur[...] = xin[u]
        row_shift = lax.rem(8 - lax.rem(me * heads, 8) - g * hpg + 8, 8)

        def batch(first):
            blocks(
                n, hpg, g, half_index, first, row_shift, order, cur, prior, gbuf, rate_ref,
                w_ref, x_ref, o_ref, mh_ref, ml_ref, st_ref,
            )

        turns = n // 2 // BATCH
        with scope("run"):
            if turns == 1:
                batch(half_index * (n // 2))
            else:
                lax.fori_loop(0, turns, lambda t, c: (batch(half_index * (n // 2) + t * BATCH), c)[1], 0)
        for earlier in range(keys - 1):
            @pl.when(u == jnp.minimum(2 * earlier + 1 + seg, units - 1))
            def _():
                forward(earlier)
        return carry

    lax.fori_loop(0, units, one_unit, 0)

    def block(h, b, state):
        g, e = h // hpg, h % hpg
        i0 = order[2 * b]
        i1 = order[2 * b + 1]
        which = lax.div(b, n // 2)
        cols = pl.ds(e * HEAD_DIM, HEAD_DIM)
        core = o_ref[h, b] + mm((mh_ref[h, b], ml_ref[h, b]), state)
        gate = jnp.concatenate([oz[g][i0, which, :, cols], oz[g][i1, which, :, cols]], axis=0).astype(f32)
        scale = lax.rsqrt(jnp.sum(core * core, axis=-1, keepdims=True) * (1.0 / HEAD_DIM) + 1e-06)
        y_ref[h, b] = (core * scale * gain_ref[0:1, :] * (gate / (1.0 + jnp.exp(-gate)))).astype(bf16)

    def target(h, source):
        return out.at[:, columns(source * width + h * HEAD_DIM, HEAD_DIM)]

    def give(h, d):
        peer = lax.rem(me + d, n)
        post(AT_Y, y_ref.at[h, peer], target(h, me), (seg, peer))

    def close(h):
        @pl.when(seg == 0)
        def _():
            inc_ref[h] = jnp.zeros((HEAD_DIM, HEAD_DIM), f32)

        @pl.when(seg == final)
        def _():
            with scope("hoplast"):
                hop(h).wait_recv()

        state = split(inc_ref[h])
        for d in range(1, n):
            block(h, lax.rem(me + d, n), state)
            if d > 1:
                give(h, d - 1)
        block(h, me, state)
        give(h, n - 1)
        pltpu.make_async_copy(y_ref.at[h, me], target(h, me), lout.at[1]).start()

    for h in range(heads):
        g = h // hpg
        late = heads - hpg
        for turn in range(late + 1):
            if h == turn:
                with scope("forward"):
                    pl.when(jnp.minimum(seg, late) == turn)(lambda: forward(keys - 1))
        if h % hpg == 0:
            pltpu.make_async_copy(oz[g].at[me], oz[g].at[me], local.at[units + 1 + g]).wait()
            with scope("zwait"):
                remote(AT_Z + g, oz[g].at[others]).wait_recv()
        with scope("close"):
            close(h)

    with scope("waity"):
        pltpu.make_async_copy(y_ref.at[:, 0], y_ref.at[:, 0], lout.at[1]).wait()
        remote(AT_Y, y_ref.at[:, others]).wait_recv()
    with scope("drain"):
        remote(AT_GATE, gbuf.at[others]).wait_send()
        for u in range(units):
            remote(u, xin.at[u, others]).wait_send()
        for g in range(keys):
            remote(AT_Z + g, oz[g].at[others]).wait_send()
        remote(AT_Y, y_ref.at[:, others]).wait_send()

        @pl.when(seg < final)
        def _():
            remote(AT_TABLE, ptab).wait_send()
            for g in range(keys):
                remote(AT_TAIL + g, otail.at[g]).wait_send()
            for h in range(heads):
                hop(h).wait_send()


def mixer(n, segs, heads, table, a_log, dt_bias, qkv, z, gates, conv_weight, gain):
    keys = max(1, heads // GROUP)
    hpg = heads // keys
    units = 2 * keys
    half = qkv.shape[0] // 2
    wide = (2 + hpg) * HEAD_DIM
    packed = (3 + hpg) // 2 * HEAD_DIM
    anywhere = pl.BlockSpec(memory_space=pl.ANY)
    vmem = pl.BlockSpec(memory_space=pltpu.VMEM)
    square = (HEAD_DIM, HEAD_DIM)
    DMA = pltpu.SemaphoreType.DMA
    kinds = units + 2 * keys + 3
    return pl.pallas_call(
        functools.partial(whole_kernel, n, segs, heads),
        out_shape=pltpu.VMEM((BLOCK, n * heads * HEAD_DIM), bf16),
        in_specs=[anywhere] * 8,
        out_specs=vmem,
        scratch_shapes=[
            pltpu.SMEM(table.shape, jnp.int32),
            pltpu.SMEM(a_log.shape, f32),
            pltpu.SMEM(dt_bias.shape, f32),
            pltpu.VMEM(gain.shape, f32),
            pltpu.VMEM((half, qkv.shape[1]), bf16),
            pltpu.VMEM(gates.shape, bf16),
            pltpu.VMEM((TAIL, qkv.shape[1]), bf16),
            pltpu.VMEM((keys, n, TAIL, packed), bf16),
            pltpu.VMEM((units, n, half, wide), bf16),
            pltpu.VMEM((keys, n, TAIL, packed), bf16),
            pltpu.VMEM((n, 2, 8, BLOCK), bf16),
            pltpu.VMEM(table.shape, jnp.int32),
            pltpu.VMEM((n, half, wide), bf16),
            pltpu.VMEM((TAIL, wide), f32),
            pltpu.VMEM((BATCH, BLOCK + 8, wide), f32),
            pltpu.VMEM((keys, CONV, wide), f32),
            pltpu.VMEM((keys, 2, 8, BLOCK), f32),
            pltpu.SMEM((2 * n,), jnp.int32),
            pltpu.VMEM((heads, n) + square, f32),
            pltpu.VMEM((heads, n) + square, bf16),
            pltpu.VMEM((heads, n) + square, bf16),
            pltpu.VMEM((keys, hpg, HEAD_DIM, 2 * HEAD_DIM), f32),
            pltpu.VMEM((heads,) + square, f32),
            pltpu.VMEM((heads,) + square, f32),
            pltpu.VMEM((heads, n) + square, bf16),
            DMA((7,)),
            DMA((units + 1 + keys,)),
            DMA((2,)),
            DMA((kinds,)),
            DMA((kinds,)),
            DMA((heads,)),
            DMA((heads,)),
            pltpu.SemaphoreType.REGULAR,
        ]
        + [pltpu.VMEM((n, 2, half, hpg * HEAD_DIM), bf16)] * keys,
        compiler_params=pltpu.CompilerParams(
            collective_id=0, has_side_effects=True, vmem_limit_bytes=48 * 1024 * 1024
        ),
        name="mixer",
    )(*[pltpu.with_memory_space_constraint(x, pltpu.HBM) for x in (table, a_log, dt_bias, qkv, z, gates, conv_weight, gain)])


def per_device(mixed_qkv, gate_z, gate_logits, block_table, conv_weight, a_log, dt_bias, norm_gain):
    n = lax.axis_size("cp")
    segs = lax.axis_size("seg")
    return mixer(
        n, segs, VALUE_HEADS // n, block_table, a_log, dt_bias, mixed_qkv, gate_z, gate_logits.T,
        conv_weight, norm_gain[None, :],
    )


def solution(mesh):
    return jax.shard_map(
        per_device,
        mesh=mesh,
        in_specs=(
            P(("seg", "cp"), None),
            P(("seg", "cp"), None),
            P(("seg", "cp"), None),
            P("seg", None),
            P(),
            P(),
            P(),
            P(),
        ),
        out_specs=P(("seg", "cp"), None),
        check_vma=False,
    )
```

```python
import functools

import jax
import jax.numpy as jnp
from jax import lax
from jax.experimental import pallas as pl
from jax.experimental.pallas import tpu as pltpu
from jax.sharding import PartitionSpec as P

VALUE_HEADS = 32
KEY_HEADS = 16
HEAD_DIM = 128
CONV = 4
BLOCK = 128
TAIL = 8
GROUP = VALUE_HEADS // KEY_HEADS
BATCH = 4

f32 = jnp.float32
bf16 = jnp.bfloat16
MESH = pl.DeviceIdType.MESH

NN = (((1,), (0,)), ((), ()))
NT = (((1,), (1,)), ((), ()))


def split(x):
    hi = x.astype(bf16)
    return hi, (x - hi.astype(f32)).astype(bf16)


def mm(a, b, dims=NN):
    def dot(x, y):
        return lax.dot_general(x, y, dims, preferred_element_type=f32)

    if dims == NT:
        return dot(a[0], b[0]) + (dot(a[0], b[1]) + dot(a[1], b[0]))
    wide = jnp.concatenate(a, axis=1)
    if b[0].shape[1] > HEAD_DIM:
        return dot(wide, jnp.concatenate([b[0], b[0]], axis=0)) + dot(a[0], b[1])
    top = jnp.concatenate([b[0], b[1]], axis=1)
    low = jnp.concatenate([b[0], jnp.zeros_like(b[1])], axis=1)
    both = dot(wide, jnp.concatenate([top, low], axis=0))
    return both[:, :HEAD_DIM] + both[:, HEAD_DIM:]


def log1p_exact(y):
    u = 1.0 + y
    return jnp.where(u == 1.0, y, jnp.log(u) * (y / jnp.where(u == 1.0, 1.0, u - 1.0)))


def scope(name):
    return jax.named_scope(name)


def squares():
    row = lax.broadcasted_iota(jnp.int32, (BLOCK, BLOCK), 0)
    col = lax.broadcasted_iota(jnp.int32, (BLOCK, BLOCK), 1)
    return row, col


def gate_terms(hpg, half_index, g, row_shift, places, gbuf, rate_ref):
    lane = lax.broadcasted_iota(jnp.int32, (8, BLOCK), 1)
    betas, decays = [], []
    for i0, i1 in places:
        one = pltpu.roll(gbuf[i0].astype(f32), (BLOCK // 2) * half_index, 1)
        two = pltpu.roll(gbuf[i1].astype(f32), (BLOCK // 2) * (1 - half_index), 1)
        found = pltpu.roll(jnp.where(lane < BLOCK // 2, one, two), row_shift, 0)
        betas.append(1.0 / (1.0 + jnp.exp(-found)))
        shifted = pltpu.roll(found, 4, 0) + rate_ref[g, 1]
        soft = jnp.maximum(shifted, 0.0) + log1p_exact(jnp.exp(-jnp.abs(shifted)))
        decays.append(rate_ref[g, 0] * soft)
    beta = jnp.concatenate(betas, axis=0)
    decay = jnp.concatenate(decays, axis=0)
    row, col = squares()
    upto = jnp.where(row <= col, 1.0, 0.0).astype(bf16)
    d0 = decay.astype(bf16)
    rest = decay - d0.astype(f32)
    d1 = rest.astype(bf16)
    d2 = (rest - d1.astype(f32)).astype(bf16)
    cum = jnp.dot(d2, upto, preferred_element_type=f32)
    cum = cum + jnp.dot(d1, upto, preferred_element_type=f32)
    cum = cum + jnp.dot(d0, upto, preferred_element_type=f32)
    count = beta.shape[0]
    spare = jnp.zeros((BLOCK - 2 * count, BLOCK), f32)
    turned = jnp.transpose(jnp.concatenate([beta, cum, spare], axis=0))
    return cum, turned, count


def prepare(hpg, blk, g, cum, turned, count, w_ref, x_ref):
    row, col = squares()
    strict = row > col
    inclusive = row >= col

    def conv(start):
        cols = slice(start, start + HEAD_DIM)
        total_rows = w_ref[g, 0:1, cols] * x_ref[5 : 5 + BLOCK, cols]
        for j in range(1, CONV):
            total_rows = total_rows + w_ref[g, j : j + 1, cols] * x_ref[5 + j : 5 + j + BLOCK, cols]
        return total_rows / (1.0 + jnp.exp(-total_rows))

    def unit(x):
        return x * lax.rsqrt(jnp.sum(x * x, axis=-1, keepdims=True) + 1e-06)

    queries = unit(conv(0)) * HEAD_DIM ** (-0.5)
    key_rows = unit(conv(HEAD_DIM))
    ks = split(key_rows)
    qs = split(queries)
    kk = mm(ks, ks, NT)
    qk = mm(qs, ks, NT)
    lower, scores, rhs, kdt, qd, last = [], [], [], [], [], []
    for e in range(hpg):
        at = blk * 8 + e
        beta = turned[:, at : at + 1]
        c = turned[:, count + at : count + at + 1]
        ct = cum[at : at + 1, :]
        final = ct[:, BLOCK - 1 :]
        spread = c - ct
        incl = jnp.where(inclusive, jnp.exp(jnp.where(inclusive, spread, 0.0)), 0.0)
        lower.append(jnp.where(strict, beta * kk * incl, 0.0))
        scores.append(split(qk * incl))
        grow = jnp.exp(c)
        values = conv((2 + e) * HEAD_DIM)
        rhs.append(split(jnp.concatenate([values * beta, key_rows * (beta * grow)], axis=1)))
        kdt.append(split(jnp.transpose(key_rows * jnp.exp(final - c))))
        qd.append(queries * grow)
        last.append(jnp.exp(final))
    return lower, scores, rhs, kdt, qd, last


def blocks(n, hpg, g, half_index, first, row_shift, order, cur, prior, gbuf, rate_ref, w_ref, x_ref, o_ref, mh_ref, ml_ref, st_ref):
    half = cur.shape[1]
    row, col = squares()
    eye = jnp.where(row == col, 1.0, 0.0).astype(f32)
    places = [(order[2 * (first + k)], order[2 * (first + k) + 1]) for k in range(BATCH)]
    cum, turned, count = gate_terms(hpg, half_index, g, row_shift, places, gbuf, rate_ref)
    lower, scores, rhs, kdt, qd, last = [], [], [], [], [], []
    for k in range(BATCH):
        b = first + k
        if k:
            x_ref[k, 0:8, :] = cur[places[k - 1][1], half - 16 :, :].astype(f32)[8:]
        else:
            ahead = order[jnp.maximum(2 * b - 1, 0)]
            near = cur[ahead, half - 16 :, :].astype(f32)[8:]
            x_ref[k, 0:8, :] = jnp.where(lax.rem(b, n // 2) == 0, prior[...], near)
        x_ref[k, 8 : 8 + half, :] = cur[places[k][0]].astype(f32)
        x_ref[k, 8 + half : 8 + 2 * half, :] = cur[places[k][1]].astype(f32)
        found = prepare(hpg, k, g, cum, turned, count, w_ref, x_ref.at[k])
        for total, more in zip((lower, scores, rhs, kdt, qd, last), found):
            total += more
    hs = range(BATCH * hpg)

    def same(size):
        return (row // size) == (col // size)

    small = 16
    power = [split(jnp.where(same(small), -lower[h], 0.0)) for h in hs]
    inverse = [eye + jnp.where(same(small), -lower[h], 0.0) for h in hs]
    steps = 1
    while 2**steps < small:
        power = [split(mm(power[h], power[h])) for h in hs]
        inverse = [inverse[h] + mm(split(inverse[h]), power[h]) for h in hs]
        steps += 1
    size = small
    while size < BLOCK:
        between = same(2 * size) & (~same(size))
        cross = [split(jnp.where(between, lower[h], 0.0)) for h in hs]
        parts = [split(inverse[h]) for h in hs]
        mixed = [split(mm(cross[h], parts[h])) for h in hs]
        inverse = [inverse[h] - mm(parts[h], mixed[h]) for h in hs]
        size *= 2
    solved = [split(mm(split(inverse[h]), rhs[h])) for h in hs]
    outs = [mm(scores[h], solved[h]) for h in hs]
    ends = [mm(kdt[h], solved[h]) for h in hs]
    readers = [split(qd[h] - outs[h][:, HEAD_DIM:]) for h in hs]
    maps = [split(last[h] * eye - ends[h][:, HEAD_DIM:]) for h in hs]
    for k in range(BATCH):
        b = first + k
        states = [split(st_ref[g, e]) for e in range(hpg)]
        for e in range(hpg):
            at = k * hpg + e
            moved = mm(maps[at], states[e])
            st_ref[g, e] = jnp.concatenate(
                [moved[:, :HEAD_DIM] + ends[at][:, :HEAD_DIM], moved[:, HEAD_DIM:]], axis=1
            )
        for e in range(hpg):
            at = k * hpg + e
            seen = mm(readers[at], states[e])
            o_ref[g * hpg + e, b] = seen[:, :HEAD_DIM] + outs[at][:, :HEAD_DIM]
            reach = split(seen[:, HEAD_DIM:])
            mh_ref[g * hpg + e, b] = reach[0]
            ml_ref[g * hpg + e, b] = reach[1]


def whole_kernel(
    n, segs, heads, table_any, a_log_any, dt_bias_any, qkv, z, gates, conv_weight, gain_any, out,
    table, a_log, dt_bias, gain_ref, stage, gstage, gsend, tstage, tsend,
    xin, otail, gbuf, ptab, cur, prior, x_ref, w_ref, rate_ref, order, o_ref, mh_ref, ml_ref, st_ref,
    inc_ref, pass_ref, y_ref, lin, lout, ssem, rsem, hsend, hrecv, ready, *oz
):
    me = lax.axis_index("cp")
    seg = lax.axis_index("seg")
    final = segs - 1
    after = lax.rem(seg + 1, segs)
    before = lax.rem(seg + segs - 1, segs)
    keys = max(1, heads // GROUP)
    hpg = heads // keys
    units = 2 * keys
    key_width = KEY_HEADS * HEAD_DIM
    width = heads * HEAD_DIM
    wz = hpg * HEAD_DIM
    rows = qkv.shape[0]
    half = rows // 2
    AT_TAIL, AT_GATE, AT_Z, AT_TABLE, AT_Y = units, units + keys, units + keys + 1, units + 2 * keys + 1, units + 2 * keys + 2

    barrier = pltpu.get_barrier_semaphore()
    for d in range(1, n):
        pl.semaphore_signal(barrier, inc=1, device_id=(seg, lax.rem(me + d, n)), device_id_type=MESH)

    @pl.when(seg < final)
    def _():
        pl.semaphore_signal(barrier, inc=1, device_id=(after, me), device_id_type=MESH)

    small = [
        pltpu.make_async_copy(src, dst, lin.at[i])
        for i, (src, dst) in enumerate(
            (
                (gates, gstage),
                (qkv.at[pl.ds(0, half)], stage),
                (qkv.at[pl.ds(rows - TAIL, TAIL)], tstage),
                (table_any, table),
                (a_log_any, a_log),
                (dt_bias_any, dt_bias),
                (gain_any, gain_ref),
            )
        )
    ]
    for copy in small:
        copy.start()

    def columns(start, size):
        return pl.ds(pl.multiple_of(start, HEAD_DIM), size)

    def places(p, g):
        key = (lax.div(p * heads, GROUP) + g) * HEAD_DIM
        value = (p * heads + g * hpg) * HEAD_DIM
        return (
            (columns(key, HEAD_DIM), pl.ds(0, HEAD_DIM)),
            (columns(key_width + key, HEAD_DIM), pl.ds(HEAD_DIM, HEAD_DIM)),
            (columns(2 * key_width + value, wz), pl.ds(2 * HEAD_DIM, wz)),
        )

    def unit_pieces(p, u, slot):
        if u % 2 == 0:
            return [(stage.at[:, src], xin.at[u, slot, :, dst]) for src, dst in places(p, u // 2)]
        return [(qkv.at[pl.ds(half, half), src], xin.at[u, slot, :, dst]) for src, dst in places(p, u // 2)]

    def gate_pieces(p, slot):
        return [(gsend.at[p], gbuf.at[slot])]

    def z_pieces(p, g, slot):
        cols = columns((p * heads + g * hpg) * HEAD_DIM, wz)
        return [(z.at[pl.ds(hf * half, half), cols], oz[g].at[slot, hf]) for hf in range(2)]

    for g in range(keys):
        for src, dst in places(me, g):
            pltpu.make_async_copy(conv_weight.at[:, src], w_ref.at[g, :, dst], lout).start()
    small[0].wait()
    line = lax.broadcasted_iota(jnp.int32, (8, BLOCK), 0)
    for p in range(n):
        tile = p * heads // 8 * 8
        shift = p * heads % 8
        strength = pltpu.roll(gstage[tile : tile + 8].astype(f32), (8 - shift) % 8, 0)
        decay = pltpu.roll(gstage[VALUE_HEADS + tile : VALUE_HEADS + tile + 8].astype(f32), (12 - shift) % 8, 0)
        gsend[p] = jnp.where(line < 4, strength, decay).astype(bf16)
    gbuf[me] = gsend[me]
    small[1].wait()
    for kind, found in [(u, unit_pieces(me, u, me)) for u in range(units)] + [
        (AT_Z + g, z_pieces(me, g, me)) for g in range(keys)
    ]:
        for src, dst in found:
            pltpu.make_async_copy(src, dst, rsem.at[kind]).start()
    with scope("entry"):
        pl.semaphore_wait(barrier, n - 1 + jnp.where(seg > 0, 1, 0))

    @pl.when(seg > 0)
    def _():
        pl.semaphore_signal(ready, inc=1, device_id=(before, me), device_id_type=MESH)

    def shared(kind):
        if not isinstance(kind, int):
            return 0
        return 0 if kind < units else 1 if kind < units + keys else kind - units - keys + 2

    def post(kind, src, dst, target):
        pltpu.make_async_remote_copy(
            src_ref=src, dst_ref=dst, send_sem=ssem.at[shared(kind)], recv_sem=rsem.at[kind],
            device_id=target, device_id_type=MESH,
        ).start()

    def remote(kind, ref):
        return pltpu.make_async_remote_copy(
            src_ref=ref, dst_ref=ref, send_sem=ssem.at[shared(kind)], recv_sem=rsem.at[kind],
            device_id=(seg, lax.rem(me + 1, n)), device_id_type=MESH,
        )

    others = pl.ds(0, n - 1)

    def post_all(kind, find):
        for d in range(1, n):
            peer = lax.rem(me + d, n)
            for src, dst in find(peer):
                post(kind, src, dst, (seg, peer))

    post_all(AT_GATE, lambda p: gate_pieces(p, me))
    post_all(0, lambda p: unit_pieces(p, 0, me))
    for copy in small[2:]:
        copy.wait()

    wide = hpg + 2
    pairs = (wide + 1) // 2
    upper = lax.broadcasted_iota(jnp.int32, (TAIL, HEAD_DIM), 0) < TAIL // 2
    for g in range(keys):
        for p in range(n):
            key = p * heads // GROUP + g
            at = [key, KEY_HEADS + key] + [2 * KEY_HEADS + p * heads + g * hpg + e for e in range(hpg)]
            tiles = [tstage[:, i * HEAD_DIM : (i + 1) * HEAD_DIM].astype(f32) for i in at]
            for i in range(pairs):
                low = tiles[i + pairs] if i + pairs < wide else tiles[i]
                both = jnp.where(upper, pltpu.roll(tiles[i], TAIL // 2, 0), low)
                tsend[g, p, :, i * HEAD_DIM : (i + 1) * HEAD_DIM] = both.astype(bf16)

    @pl.when(seg < final)
    def _():
        with scope("readywait"):
            pl.semaphore_wait(ready, 1)
        post(AT_TABLE, table_any, ptab, (after, me))
        for g in range(keys):
            for d in range(n):
                peer = lax.rem(me + d, n)
                post(AT_TAIL + g, tsend.at[g, peer], otail.at[g, me], (after, peer))

    for u in range(1, units):
        post_all(u, lambda p: unit_pieces(p, u, me))
    for g in range(keys):
        post_all(AT_Z + g, lambda p: z_pieces(p, g, me))

    def find(b, carry):
        parity = lax.div(b, n)
        place = jnp.int32(0)
        for j in range(n):
            place = jnp.where(table[0, 2 * j + parity] == b, j, place)
        order[b] = place
        return carry

    lax.fori_loop(0, 2 * n, find, 0)

    row, col = squares()
    for g in range(keys):
        scale = jnp.zeros((8, BLOCK), f32)
        shift = jnp.zeros((8, BLOCK), f32)
        for e in range(hpg):
            h = me * heads + g * hpg + e
            scale = jnp.where(line == e, a_log[h], scale)
            shift = jnp.where(line == e, dt_bias[h], shift)
            st_ref[g, e, :, :HEAD_DIM] = jnp.zeros((HEAD_DIM, HEAD_DIM), f32)
            st_ref[g, e, :, HEAD_DIM:] = jnp.where(row == col, 1.0, 0.0).astype(f32)
        rate_ref[g, 0] = -jnp.exp(scale)
        rate_ref[g, 1] = shift

    pltpu.make_async_copy(w_ref, w_ref, lout).wait()
    with scope("gatewait"):
        remote(AT_GATE, gbuf.at[others]).wait_recv()

    @pl.when(seg > 0)
    def _():
        remote(AT_TABLE, ptab).wait_recv()

    def hop(h):
        return pltpu.make_async_remote_copy(
            src_ref=pass_ref.at[h],
            dst_ref=inc_ref.at[h],
            send_sem=hsend,
            recv_sem=hrecv.at[h],
            device_id=(after, me),
            device_id_type=MESH,
        )

    def forward(g):
        @pl.when((seg == 0) & (seg < final))
        def _():
            for e in range(hpg):
                h = g * hpg + e
                pass_ref[h] = st_ref[g, e, :, :HEAD_DIM]
                hop(h).start()

        @pl.when((seg > 0) & (seg < final))
        def _():
            for e in range(hpg):
                h = g * hpg + e
                through = split(st_ref[g, e, :, HEAD_DIM:])
                with scope("hopmid"):
                    hop(h).wait_recv()
                pass_ref[h] = st_ref[g, e, :, :HEAD_DIM] + mm(through, split(inc_ref[h]))
                hop(h).start()

    def one_unit(u, carry):
        g = lax.div(u, 2)
        half_index = lax.rem(u, 2)
        with scope("unitwait"):
            remote(u, xin.at[u]).wait_recv()

        @pl.when((half_index == 0) & (seg == 0))
        def _():
            prior[...] = jnp.zeros_like(prior)

        @pl.when((half_index == 0) & (seg > 0))
        def _():
            with scope("tailwait"):
                remote(AT_TAIL + g, otail.at[g]).wait_recv()
            found = jnp.zeros(otail.shape[2:], f32)
            for j in range(n):
                hit = ptab[0:1, 2 * j + 1 : 2 * j + 2] == 2 * n - 1
                found = jnp.where(hit, otail[g, j].astype(f32), found)
            for i in range(wide):
                pair = found[:, i % pairs * HEAD_DIM : (i % pairs + 1) * HEAD_DIM]
                prior[:, i * HEAD_DIM : (i + 1) * HEAD_DIM] = pltpu.roll(pair, TAIL // 2, 0) if i < pairs else pair

        @pl.when(half_index == 1)
        def _():
            prior[...] = cur[order[n - 1], half - 16 :, :].astype(f32)[8:]

        cur[...] = xin[u]
        row_shift = lax.rem(8 - g * hpg, 8)

        def batch(first):
            blocks(
                n, hpg, g, half_index, first, row_shift, order, cur, prior, gbuf, rate_ref,
                w_ref, x_ref, o_ref, mh_ref, ml_ref, st_ref,
            )

        turns = n // 2 // BATCH
        with scope("run"):
            if turns == 1:
                batch(half_index * (n // 2))
            else:
                lax.fori_loop(0, turns, lambda t, c: (batch(half_index * (n // 2) + t * BATCH), c)[1], 0)
        for earlier in range(keys - 1):
            @pl.when(u == jnp.minimum(2 * earlier + 1 + seg, units - 1))
            def _():
                forward(earlier)
        return carry

    lax.fori_loop(0, units, one_unit, 0)

    def block(h, b, state):
        g, e = h // hpg, h % hpg
        i0 = order[2 * b]
        i1 = order[2 * b + 1]
        which = lax.div(b, n // 2)
        cols = pl.ds(e * HEAD_DIM, HEAD_DIM)
        core = o_ref[h, b] + mm((mh_ref[h, b], ml_ref[h, b]), state)
        gate = jnp.concatenate([oz[g][i0, which, :, cols], oz[g][i1, which, :, cols]], axis=0).astype(f32)
        scale = lax.rsqrt(jnp.sum(core * core, axis=-1, keepdims=True) * (1.0 / HEAD_DIM) + 1e-06)
        y_ref[h, b] = (core * scale * gain_ref[0:1, :] * (gate / (1.0 + jnp.exp(-gate)))).astype(bf16)

    def target(h, source):
        return out.at[:, columns(source * width + h * HEAD_DIM, HEAD_DIM)]

    def give(h, d):
        peer = lax.rem(me + d, n)
        post(AT_Y, y_ref.at[h, peer], target(h, me), (seg, peer))

    def close(h):
        @pl.when(seg == 0)
        def _():
            inc_ref[h] = jnp.zeros((HEAD_DIM, HEAD_DIM), f32)

        @pl.when((seg == final) & (seg > 0))
        def _():
            with scope("hoplast"):
                hop(h).wait_recv()

        state = split(inc_ref[h])
        for d in range(1, n):
            block(h, lax.rem(me + d, n), state)
            if d > 1:
                give(h, d - 1)
        block(h, me, state)
        give(h, n - 1)
        pltpu.make_async_copy(y_ref.at[h, me], target(h, me), rsem.at[AT_Y]).start()

    for h in range(heads):
        g = h // hpg
        late = heads - hpg
        for turn in range(late + 1):
            if h == turn:
                with scope("forward"):
                    pl.when(jnp.minimum(seg, late) == turn)(lambda: forward(keys - 1))
        if h % hpg == 0:
            with scope("zwait"):
                remote(AT_Z + g, oz[g]).wait_recv()
        with scope("close"):
            close(h)

    with scope("waity"):
        remote(AT_Y, y_ref).wait_recv()
    with scope("drain"):
        remote(AT_GATE, gbuf.at[others]).wait_send()
        remote(0, xin.at[:, others]).wait_send()
        for g in range(keys):
            remote(AT_Z + g, oz[g].at[others]).wait_send()
        remote(AT_Y, y_ref.at[:, others]).wait_send()

        @pl.when(seg < final)
        def _():
            remote(AT_TABLE, ptab).wait_send()
            remote(AT_TAIL, otail).wait_send()
            pltpu.make_async_remote_copy(
                src_ref=pass_ref, dst_ref=inc_ref, send_sem=hsend, recv_sem=hrecv.at[0],
                device_id=(after, me), device_id_type=MESH,
            ).wait_send()


def mixer(n, segs, heads, table, a_log, dt_bias, qkv, z, gates, conv_weight, gain):
    keys = max(1, heads // GROUP)
    hpg = heads // keys
    units = 2 * keys
    half = qkv.shape[0] // 2
    wide = (2 + hpg) * HEAD_DIM
    packed = (3 + hpg) // 2 * HEAD_DIM
    anywhere = pl.BlockSpec(memory_space=pl.ANY)
    vmem = pl.BlockSpec(memory_space=pltpu.VMEM)
    square = (HEAD_DIM, HEAD_DIM)
    DMA = pltpu.SemaphoreType.DMA
    kinds = units + 2 * keys + 3
    return pl.pallas_call(
        functools.partial(whole_kernel, n, segs, heads),
        out_shape=pltpu.VMEM((BLOCK, n * heads * HEAD_DIM), bf16),
        in_specs=[anywhere] * 8,
        out_specs=vmem,
        scratch_shapes=[
            pltpu.SMEM(table.shape, jnp.int32),
            pltpu.SMEM(a_log.shape, f32),
            pltpu.SMEM(dt_bias.shape, f32),
            pltpu.VMEM(gain.shape, f32),
            pltpu.VMEM((half, qkv.shape[1]), bf16),
            pltpu.VMEM(gates.shape, bf16),
            pltpu.VMEM((n, 8, BLOCK), bf16),
            pltpu.VMEM((TAIL, qkv.shape[1]), bf16),
            pltpu.VMEM((keys, n, TAIL, packed), bf16),
            pltpu.VMEM((units, n, half, wide), bf16),
            pltpu.VMEM((keys, n, TAIL, packed), bf16),
            pltpu.VMEM((n, 8, BLOCK), bf16),
            pltpu.VMEM(table.shape, jnp.int32),
            pltpu.VMEM((n, half, wide), bf16),
            pltpu.VMEM((TAIL, wide), f32),
            pltpu.VMEM((BATCH, BLOCK + 8, wide), f32),
            pltpu.VMEM((keys, CONV, wide), f32),
            pltpu.VMEM((keys, 2, 8, BLOCK), f32),
            pltpu.SMEM((2 * n,), jnp.int32),
            pltpu.VMEM((heads, n) + square, f32),
            pltpu.VMEM((heads, n) + square, bf16),
            pltpu.VMEM((heads, n) + square, bf16),
            pltpu.VMEM((keys, hpg, HEAD_DIM, 2 * HEAD_DIM), f32),
            pltpu.VMEM((heads,) + square, f32),
            pltpu.VMEM((heads,) + square, f32),
            pltpu.VMEM((heads, n) + square, bf16),
            DMA((7,)),
            DMA,
            DMA((kinds - units - keys + 2,)),
            DMA((kinds,)),
            DMA,
            DMA((heads,)),
            pltpu.SemaphoreType.REGULAR,
        ]
        + [pltpu.VMEM((n, 2, half, hpg * HEAD_DIM), bf16)] * keys,
        compiler_params=pltpu.CompilerParams(
            collective_id=0, has_side_effects=True, vmem_limit_bytes=48 * 1024 * 1024
        ),
        name="mixer",
    )(*[pltpu.with_memory_space_constraint(x, pltpu.HBM) for x in (table, a_log, dt_bias, qkv, z, gates, conv_weight, gain)])


def per_device(mixed_qkv, gate_z, gate_logits, block_table, conv_weight, a_log, dt_bias, norm_gain):
    n = lax.axis_size("cp")
    segs = lax.axis_size("seg")
    return mixer(
        n, segs, VALUE_HEADS // n, block_table, a_log, dt_bias, mixed_qkv, gate_z, gate_logits.T,
        conv_weight, norm_gain[None, :],
    )


def solution(mesh):
    return jax.shard_map(
        per_device,
        mesh=mesh,
        in_specs=(
            P(("seg", "cp"), None),
            P(("seg", "cp"), None),
            P(("seg", "cp"), None),
            P("seg", None),
            P(),
            P(),
            P(),
            P(),
        ),
        out_specs=P(("seg", "cp"), None),
        check_vma=False,
    )
```

```python
import functools

import jax
import jax.numpy as jnp
from jax import lax
from jax.experimental import pallas as pl
from jax.experimental.pallas import tpu as pltpu
from jax.sharding import PartitionSpec as P

VALUE_HEADS = 32
KEY_HEADS = 16
HEAD_DIM = 128
CONV = 4
BLOCK = 128
TAIL = 8
GROUP = VALUE_HEADS // KEY_HEADS
BATCH = 4

f32 = jnp.float32
bf16 = jnp.bfloat16
MESH = pl.DeviceIdType.MESH

NN = (((1,), (0,)), ((), ()))
NT = (((1,), (1,)), ((), ()))


def split(x):
    hi = x.astype(bf16)
    return hi, (x - hi.astype(f32)).astype(bf16)


def mm(a, b, dims=NN):
    def dot(x, y):
        return lax.dot_general(x, y, dims, preferred_element_type=f32)

    if dims == NT:
        return dot(a[0], b[0]) + (dot(a[0], b[1]) + dot(a[1], b[0]))
    wide = jnp.concatenate(a, axis=1)
    if b[0].shape[1] > HEAD_DIM:
        return dot(wide, jnp.concatenate([b[0], b[0]], axis=0)) + dot(a[0], b[1])
    top = jnp.concatenate([b[0], b[1]], axis=1)
    low = jnp.concatenate([b[0], jnp.zeros_like(b[1])], axis=1)
    both = dot(wide, jnp.concatenate([top, low], axis=0))
    return both[:, :HEAD_DIM] + both[:, HEAD_DIM:]


def log1p_exact(y):
    u = 1.0 + y
    return jnp.where(u == 1.0, y, jnp.log(u) * (y / jnp.where(u == 1.0, 1.0, u - 1.0)))


def scope(name):
    return jax.named_scope(name)


def squares():
    row = lax.broadcasted_iota(jnp.int32, (BLOCK, BLOCK), 0)
    col = lax.broadcasted_iota(jnp.int32, (BLOCK, BLOCK), 1)
    return row, col


def gate_terms(hpg, half_index, g, row_shift, places, gbuf, rate_ref):
    lane = lax.broadcasted_iota(jnp.int32, (8, BLOCK), 1)
    betas, decays = [], []
    for i0, i1 in places:
        one = pltpu.roll(gbuf[i0].astype(f32), (BLOCK // 2) * half_index, 1)
        two = pltpu.roll(gbuf[i1].astype(f32), (BLOCK // 2) * (1 - half_index), 1)
        found = pltpu.roll(jnp.where(lane < BLOCK // 2, one, two), row_shift, 0)
        betas.append(1.0 / (1.0 + jnp.exp(-found)))
        shifted = pltpu.roll(found, 4, 0) + rate_ref[g, 1]
        soft = jnp.maximum(shifted, 0.0) + log1p_exact(jnp.exp(-jnp.abs(shifted)))
        decays.append(rate_ref[g, 0] * soft)
    beta = jnp.concatenate(betas, axis=0)
    decay = jnp.concatenate(decays, axis=0)
    row, col = squares()
    upto = jnp.where(row <= col, 1.0, 0.0).astype(bf16)
    d0 = decay.astype(bf16)
    rest = decay - d0.astype(f32)
    d1 = rest.astype(bf16)
    d2 = (rest - d1.astype(f32)).astype(bf16)
    cum = jnp.dot(d2, upto, preferred_element_type=f32)
    cum = cum + jnp.dot(d1, upto, preferred_element_type=f32)
    cum = cum + jnp.dot(d0, upto, preferred_element_type=f32)
    count = beta.shape[0]
    spare = jnp.zeros((BLOCK - 2 * count, BLOCK), f32)
    turned = jnp.transpose(jnp.concatenate([beta, cum, spare], axis=0))
    return cum, turned, count


def prepare(hpg, blk, g, cum, turned, count, w_ref, x_ref):
    row, col = squares()
    strict = row > col
    inclusive = row >= col

    def conv(start):
        cols = slice(start, start + HEAD_DIM)
        total_rows = w_ref[g, 0:1, cols] * x_ref[5 : 5 + BLOCK, cols]
        for j in range(1, CONV):
            total_rows = total_rows + w_ref[g, j : j + 1, cols] * x_ref[5 + j : 5 + j + BLOCK, cols]
        return total_rows / (1.0 + jnp.exp(-total_rows))

    def unit(x):
        return x * lax.rsqrt(jnp.sum(x * x, axis=-1, keepdims=True) + 1e-06)

    queries = unit(conv(0)) * HEAD_DIM ** (-0.5)
    key_rows = unit(conv(HEAD_DIM))
    ks = split(key_rows)
    qs = split(queries)
    kk = mm(ks, ks, NT)
    qk = mm(qs, ks, NT)
    lower, scores, rhs, kdt, qd, last = [], [], [], [], [], []
    for e in range(hpg):
        at = blk * 8 + e
        beta = turned[:, at : at + 1]
        c = turned[:, count + at : count + at + 1]
        ct = cum[at : at + 1, :]
        final = ct[:, BLOCK - 1 :]
        spread = c - ct
        incl = jnp.where(inclusive, jnp.exp(jnp.where(inclusive, spread, 0.0)), 0.0)
        lower.append(jnp.where(strict, beta * kk * incl, 0.0))
        scores.append(split(qk * incl))
        grow = jnp.exp(c)
        values = conv((2 + e) * HEAD_DIM)
        rhs.append(split(jnp.concatenate([values * beta, key_rows * (beta * grow)], axis=1)))
        kdt.append(split(jnp.transpose(key_rows * jnp.exp(final - c))))
        qd.append(queries * grow)
        last.append(jnp.exp(final))
    return lower, scores, rhs, kdt, qd, last


def blocks(n, hpg, g, half_index, first, row_shift, order, cur, prior, gbuf, rate_ref, w_ref, x_ref, o_ref, mh_ref, ml_ref, st_ref):
    half = cur.shape[1]
    row, col = squares()
    eye = jnp.where(row == col, 1.0, 0.0).astype(f32)
    places = [(order[2 * (first + k)], order[2 * (first + k) + 1]) for k in range(BATCH)]
    cum, turned, count = gate_terms(hpg, half_index, g, row_shift, places, gbuf, rate_ref)
    lower, scores, rhs, kdt, qd, last = [], [], [], [], [], []
    for k in range(BATCH):
        b = first + k
        if k:
            x_ref[k, 0:8, :] = cur[places[k - 1][1], half - 16 :, :].astype(f32)[8:]
        else:
            ahead = order[jnp.maximum(2 * b - 1, 0)]
            near = cur[ahead, half - 16 :, :].astype(f32)[8:]
            x_ref[k, 0:8, :] = jnp.where(lax.rem(b, n // 2) == 0, prior[...], near)
        x_ref[k, 8 : 8 + half, :] = cur[places[k][0]].astype(f32)
        x_ref[k, 8 + half : 8 + 2 * half, :] = cur[places[k][1]].astype(f32)
        found = prepare(hpg, k, g, cum, turned, count, w_ref, x_ref.at[k])
        for total, more in zip((lower, scores, rhs, kdt, qd, last), found):
            total += more
    hs = range(BATCH * hpg)

    def same(size):
        return (row // size) == (col // size)

    small = 16
    power = [split(jnp.where(same(small), -lower[h], 0.0)) for h in hs]
    inverse = [eye + jnp.where(same(small), -lower[h], 0.0) for h in hs]
    steps = 1
    while 2**steps < small:
        power = [split(mm(power[h], power[h])) for h in hs]
        inverse = [inverse[h] + mm(split(inverse[h]), power[h]) for h in hs]
        steps += 1
    size = small
    while size < BLOCK:
        between = same(2 * size) & (~same(size))
        cross = [split(jnp.where(between, lower[h], 0.0)) for h in hs]
        parts = [split(inverse[h]) for h in hs]
        mixed = [split(mm(cross[h], parts[h])) for h in hs]
        inverse = [inverse[h] - mm(parts[h], mixed[h]) for h in hs]
        size *= 2
    solved = [split(mm(split(inverse[h]), rhs[h])) for h in hs]
    outs = [mm(scores[h], solved[h]) for h in hs]
    ends = [mm(kdt[h], solved[h]) for h in hs]
    readers = [split(qd[h] - outs[h][:, HEAD_DIM:]) for h in hs]
    maps = [split(last[h] * eye - ends[h][:, HEAD_DIM:]) for h in hs]
    for k in range(BATCH):
        b = first + k
        states = [split(st_ref[g, e]) for e in range(hpg)]
        for e in range(hpg):
            at = k * hpg + e
            moved = mm(maps[at], states[e])
            st_ref[g, e] = jnp.concatenate(
                [moved[:, :HEAD_DIM] + ends[at][:, :HEAD_DIM], moved[:, HEAD_DIM:]], axis=1
            )
        for e in range(hpg):
            at = k * hpg + e
            seen = mm(readers[at], states[e])
            o_ref[g * hpg + e, b] = seen[:, :HEAD_DIM] + outs[at][:, :HEAD_DIM]
            reach = split(seen[:, HEAD_DIM:])
            mh_ref[g * hpg + e, b] = reach[0]
            ml_ref[g * hpg + e, b] = reach[1]


def whole_kernel(
    n, segs, heads, table_any, a_log_any, dt_bias_any, qkv, z, gates, conv_weight, gain_any, out,
    table, a_log, dt_bias, gain_ref, stage, gstage, gsend, tstage, tsend,
    xin, otail, gbuf, ptab, cur, prior, x_ref, w_ref, rate_ref, order, o_ref, mh_ref, ml_ref, st_ref,
    inc_ref, pass_ref, y_ref, lin, lout, ssem, rsem, hsend, hrecv, ready, *oz
):
    me = lax.axis_index("cp")
    seg = lax.axis_index("seg")
    final = segs - 1
    after = lax.rem(seg + 1, segs)
    before = lax.rem(seg + segs - 1, segs)
    keys = max(1, heads // GROUP)
    hpg = heads // keys
    units = 2 * keys
    key_width = KEY_HEADS * HEAD_DIM
    width = heads * HEAD_DIM
    wz = hpg * HEAD_DIM
    rows = qkv.shape[0]
    half = rows // 2
    AT_TAIL, AT_GATE, AT_Z, AT_TABLE, AT_Y = units, units + keys, units + keys + 1, units + 2 * keys + 1, units + 2 * keys + 2

    barrier = pltpu.get_barrier_semaphore()
    for d in range(1, n):
        pl.semaphore_signal(barrier, inc=1, device_id=(seg, lax.rem(me + d, n)), device_id_type=MESH)

    @pl.when(seg < final)
    def _():
        pl.semaphore_signal(barrier, inc=1, device_id=(after, me), device_id_type=MESH)

    small = [
        pltpu.make_async_copy(src, dst, lin.at[i])
        for i, (src, dst) in enumerate(
            (
                (gates, gstage),
                (qkv.at[pl.ds(0, half)], stage),
                (qkv.at[pl.ds(rows - TAIL, TAIL)], tstage),
                (table_any, table),
                (a_log_any, a_log),
                (dt_bias_any, dt_bias),
                (gain_any, gain_ref),
            )
        )
    ]
    for copy in small:
        copy.start()

    def columns(start, size):
        return pl.ds(pl.multiple_of(start, HEAD_DIM), size)

    def places(p, g):
        key = (lax.div(p * heads, GROUP) + g) * HEAD_DIM
        value = (p * heads + g * hpg) * HEAD_DIM
        return (
            (columns(key, HEAD_DIM), pl.ds(0, HEAD_DIM)),
            (columns(key_width + key, HEAD_DIM), pl.ds(HEAD_DIM, HEAD_DIM)),
            (columns(2 * key_width + value, wz), pl.ds(2 * HEAD_DIM, wz)),
        )

    def unit_pieces(p, u, slot):
        if u % 2 == 0:
            return [(stage.at[:, src], xin.at[u, slot, :, dst]) for src, dst in places(p, u // 2)]
        return [(qkv.at[pl.ds(half, half), src], xin.at[u, slot, :, dst]) for src, dst in places(p, u // 2)]

    def gate_pieces(p, slot):
        return [(gsend.at[p], gbuf.at[slot])]

    def z_pieces(p, g, slot):
        cols = columns((p * heads + g * hpg) * HEAD_DIM, wz)
        return [(z.at[pl.ds(hf * half, half), cols], oz[g].at[slot, hf]) for hf in range(2)]

    for g in range(keys):
        for src, dst in places(me, g):
            pltpu.make_async_copy(conv_weight.at[:, src], w_ref.at[g, :, dst], lout).start()
    small[0].wait()
    line = lax.broadcasted_iota(jnp.int32, (8, BLOCK), 0)
    for p in range(n):
        tile = p * heads // 8 * 8
        shift = p * heads % 8
        strength = pltpu.roll(gstage[tile : tile + 8].astype(f32), (8 - shift) % 8, 0)
        decay = pltpu.roll(gstage[VALUE_HEADS + tile : VALUE_HEADS + tile + 8].astype(f32), (12 - shift) % 8, 0)
        gsend[p] = jnp.where(line < 4, strength, decay).astype(bf16)
    gbuf[me] = gsend[me]
    small[1].wait()
    for kind, found in [(u, unit_pieces(me, u, me)) for u in range(units)] + [
        (AT_Z + g, z_pieces(me, g, me)) for g in range(keys)
    ]:
        for src, dst in found:
            pltpu.make_async_copy(src, dst, rsem.at[kind]).start()
    with scope("entry"):
        pl.semaphore_wait(barrier, n - 1 + jnp.where(seg > 0, 1, 0))

    @pl.when(seg > 0)
    def _():
        pl.semaphore_signal(ready, inc=1, device_id=(before, me), device_id_type=MESH)

    def shared(kind):
        if not isinstance(kind, int):
            return 0
        return 0 if kind < units else 1 if kind < units + keys else kind - units - keys + 2

    def post(kind, src, dst, target):
        pltpu.make_async_remote_copy(
            src_ref=src, dst_ref=dst, send_sem=ssem.at[shared(kind)], recv_sem=rsem.at[kind],
            device_id=target, device_id_type=MESH,
        ).start()

    def remote(kind, ref):
        return pltpu.make_async_remote_copy(
            src_ref=ref, dst_ref=ref, send_sem=ssem.at[shared(kind)], recv_sem=rsem.at[kind],
            device_id=(seg, lax.rem(me + 1, n)), device_id_type=MESH,
        )

    others = pl.ds(0, n - 1)

    def post_all(kind, find):
        for d in range(1, n):
            peer = lax.rem(me + d, n)
            for src, dst in find(peer):
                post(kind, src, dst, (seg, peer))

    post_all(AT_GATE, lambda p: gate_pieces(p, me))
    post_all(0, lambda p: unit_pieces(p, 0, me))
    for copy in small[2:]:
        copy.wait()

    wide = hpg + 2
    pairs = (wide + 1) // 2
    upper = lax.broadcasted_iota(jnp.int32, (TAIL, HEAD_DIM), 0) < TAIL // 2
    for g in range(keys):
        for p in range(n):
            key = p * heads // GROUP + g
            at = [key, KEY_HEADS + key] + [2 * KEY_HEADS + p * heads + g * hpg + e for e in range(hpg)]
            tiles = [tstage[:, i * HEAD_DIM : (i + 1) * HEAD_DIM].astype(f32) for i in at]
            for i in range(pairs):
                low = tiles[i + pairs] if i + pairs < wide else tiles[i]
                both = jnp.where(upper, pltpu.roll(tiles[i], TAIL // 2, 0), low)
                tsend[g, p, :, i * HEAD_DIM : (i + 1) * HEAD_DIM] = both.astype(bf16)

    def find(b, carry):
        parity = lax.div(b, n)
        place = jnp.int32(0)
        for j in range(n):
            place = jnp.where(table[0, 2 * j + parity] == b, j, place)
        order[b] = place
        return carry

    lax.fori_loop(0, 2 * n, find, 0)

    row, col = squares()
    for g in range(keys):
        scale = jnp.zeros((8, BLOCK), f32)
        shift = jnp.zeros((8, BLOCK), f32)
        for e in range(hpg):
            h = me * heads + g * hpg + e
            scale = jnp.where(line == e, a_log[h], scale)
            shift = jnp.where(line == e, dt_bias[h], shift)
            st_ref[g, e, :, :HEAD_DIM] = jnp.zeros((HEAD_DIM, HEAD_DIM), f32)
            st_ref[g, e, :, HEAD_DIM:] = jnp.where(row == col, 1.0, 0.0).astype(f32)
        rate_ref[g, 0] = -jnp.exp(scale)
        rate_ref[g, 1] = shift

    @pl.when(seg < final)
    def _():
        with scope("readywait"):
            pl.semaphore_wait(ready, 1)
        post(AT_TABLE, table_any, ptab, (after, me))
        for g in range(keys):
            for d in range(n):
                peer = lax.rem(me + d, n)
                post(AT_TAIL + g, tsend.at[g, peer], otail.at[g, me], (after, peer))

    for u in range(1, units):
        post_all(u, lambda p: unit_pieces(p, u, me))
    for g in range(keys):
        post_all(AT_Z + g, lambda p: z_pieces(p, g, me))

    pltpu.make_async_copy(w_ref, w_ref, lout).wait()
    with scope("gatewait"):
        remote(AT_GATE, gbuf.at[others]).wait_recv()

    @pl.when(seg > 0)
    def _():
        remote(AT_TABLE, ptab).wait_recv()

    def hop(h):
        return pltpu.make_async_remote_copy(
            src_ref=pass_ref.at[h],
            dst_ref=inc_ref.at[h],
            send_sem=hsend,
            recv_sem=hrecv.at[h],
            device_id=(after, me),
            device_id_type=MESH,
        )

    def forward(g):
        @pl.when((seg == 0) & (seg < final))
        def _():
            for e in range(hpg):
                h = g * hpg + e
                pass_ref[h] = st_ref[g, e, :, :HEAD_DIM]
                hop(h).start()

        @pl.when((seg > 0) & (seg < final))
        def _():
            for e in range(hpg):
                h = g * hpg + e
                through = split(st_ref[g, e, :, HEAD_DIM:])
                with scope("hopmid"):
                    hop(h).wait_recv()
                pass_ref[h] = st_ref[g, e, :, :HEAD_DIM] + mm(through, split(inc_ref[h]))
                hop(h).start()

    def one_unit(u, carry):
        g = lax.div(u, 2)
        half_index = lax.rem(u, 2)
        with scope("unitwait"):
            remote(u, xin.at[u]).wait_recv()

        @pl.when((half_index == 0) & (seg == 0))
        def _():
            prior[...] = jnp.zeros_like(prior)

        @pl.when((half_index == 0) & (seg > 0))
        def _():
            with scope("tailwait"):
                remote(AT_TAIL + g, otail.at[g]).wait_recv()
            found = jnp.zeros(otail.shape[2:], f32)
            for j in range(n):
                hit = ptab[0:1, 2 * j + 1 : 2 * j + 2] == 2 * n - 1
                found = jnp.where(hit, otail[g, j].astype(f32), found)
            for i in range(wide):
                pair = found[:, i % pairs * HEAD_DIM : (i % pairs + 1) * HEAD_DIM]
                prior[:, i * HEAD_DIM : (i + 1) * HEAD_DIM] = pltpu.roll(pair, TAIL // 2, 0) if i < pairs else pair

        @pl.when(half_index == 1)
        def _():
            prior[...] = cur[order[n - 1], half - 16 :, :].astype(f32)[8:]

        cur[...] = xin[u]
        row_shift = lax.rem(8 - g * hpg, 8)

        def batch(first):
            blocks(
                n, hpg, g, half_index, first, row_shift, order, cur, prior, gbuf, rate_ref,
                w_ref, x_ref, o_ref, mh_ref, ml_ref, st_ref,
            )

        turns = n // 2 // BATCH
        with scope("run"):
            if turns == 1:
                batch(half_index * (n // 2))
            else:
                lax.fori_loop(0, turns, lambda t, c: (batch(half_index * (n // 2) + t * BATCH), c)[1], 0)
        for earlier in range(keys - 1):
            @pl.when(u == jnp.minimum(2 * earlier + 1 + seg, units - 1))
            def _():
                forward(earlier)
        return carry

    lax.fori_loop(0, units, one_unit, 0)

    def block(h, b, state):
        g, e = h // hpg, h % hpg
        i0 = order[2 * b]
        i1 = order[2 * b + 1]
        which = lax.div(b, n // 2)
        cols = pl.ds(e * HEAD_DIM, HEAD_DIM)
        core = o_ref[h, b] + mm((mh_ref[h, b], ml_ref[h, b]), state)
        gate = jnp.concatenate([oz[g][i0, which, :, cols], oz[g][i1, which, :, cols]], axis=0).astype(f32)
        scale = lax.rsqrt(jnp.sum(core * core, axis=-1, keepdims=True) * (1.0 / HEAD_DIM) + 1e-06)
        y_ref[h, b] = (core * scale * gain_ref[0:1, :] * (gate / (1.0 + jnp.exp(-gate)))).astype(bf16)

    def target(h, source):
        return out.at[:, columns(source * width + h * HEAD_DIM, HEAD_DIM)]

    def give(h, d):
        peer = lax.rem(me + d, n)
        post(AT_Y, y_ref.at[h, peer], target(h, me), (seg, peer))

    def close(h):
        @pl.when(seg == 0)
        def _():
            inc_ref[h] = jnp.zeros((HEAD_DIM, HEAD_DIM), f32)

        @pl.when((seg == final) & (seg > 0))
        def _():
            with scope("hoplast"):
                hop(h).wait_recv()

        state = split(inc_ref[h])
        for d in range(1, n):
            block(h, lax.rem(me + d, n), state)
            if d > 1:
                give(h, d - 1)
        block(h, me, state)
        give(h, n - 1)
        pltpu.make_async_copy(y_ref.at[h, me], target(h, me), rsem.at[AT_Y]).start()

    for h in range(heads):
        g = h // hpg
        late = heads - hpg
        for turn in range(late + 1):
            if h == turn:
                with scope("forward"):
                    pl.when(jnp.minimum(seg, late) == turn)(lambda: forward(keys - 1))
        if h % hpg == 0:
            with scope("zwait"):
                remote(AT_Z + g, oz[g]).wait_recv()
        with scope("close"):
            close(h)

    with scope("waity"):
        remote(AT_Y, y_ref).wait_recv()
    with scope("drain"):
        remote(AT_GATE, gbuf.at[others]).wait_send()
        remote(0, xin.at[:, others]).wait_send()
        for g in range(keys):
            remote(AT_Z + g, oz[g].at[others]).wait_send()
        remote(AT_Y, y_ref.at[:, others]).wait_send()

        @pl.when(seg < final)
        def _():
            remote(AT_TABLE, ptab).wait_send()
            remote(AT_TAIL, otail).wait_send()
            pltpu.make_async_remote_copy(
                src_ref=pass_ref, dst_ref=inc_ref, send_sem=hsend, recv_sem=hrecv.at[0],
                device_id=(after, me), device_id_type=MESH,
            ).wait_send()


def mixer(n, segs, heads, table, a_log, dt_bias, qkv, z, gates, conv_weight, gain):
    keys = max(1, heads // GROUP)
    hpg = heads // keys
    units = 2 * keys
    half = qkv.shape[0] // 2
    wide = (2 + hpg) * HEAD_DIM
    packed = (3 + hpg) // 2 * HEAD_DIM
    anywhere = pl.BlockSpec(memory_space=pl.ANY)
    vmem = pl.BlockSpec(memory_space=pltpu.VMEM)
    square = (HEAD_DIM, HEAD_DIM)
    DMA = pltpu.SemaphoreType.DMA
    kinds = units + 2 * keys + 3
    return pl.pallas_call(
        functools.partial(whole_kernel, n, segs, heads),
        out_shape=pltpu.VMEM((BLOCK, n * heads * HEAD_DIM), bf16),
        in_specs=[anywhere] * 8,
        out_specs=vmem,
        scratch_shapes=[
            pltpu.SMEM(table.shape, jnp.int32),
            pltpu.SMEM(a_log.shape, f32),
            pltpu.SMEM(dt_bias.shape, f32),
            pltpu.VMEM(gain.shape, f32),
            pltpu.VMEM((half, qkv.shape[1]), bf16),
            pltpu.VMEM(gates.shape, bf16),
            pltpu.VMEM((n, 8, BLOCK), bf16),
            pltpu.VMEM((TAIL, qkv.shape[1]), bf16),
            pltpu.VMEM((keys, n, TAIL, packed), bf16),
            pltpu.VMEM((units, n, half, wide), bf16),
            pltpu.VMEM((keys, n, TAIL, packed), bf16),
            pltpu.VMEM((n, 8, BLOCK), bf16),
            pltpu.VMEM(table.shape, jnp.int32),
            pltpu.VMEM((n, half, wide), bf16),
            pltpu.VMEM((TAIL, wide), f32),
            pltpu.VMEM((BATCH, BLOCK + 8, wide), f32),
            pltpu.VMEM((keys, CONV, wide), f32),
            pltpu.VMEM((keys, 2, 8, BLOCK), f32),
            pltpu.SMEM((2 * n,), jnp.int32),
            pltpu.VMEM((heads, n) + square, f32),
            pltpu.VMEM((heads, n) + square, bf16),
            pltpu.VMEM((heads, n) + square, bf16),
            pltpu.VMEM((keys, hpg, HEAD_DIM, 2 * HEAD_DIM), f32),
            pltpu.VMEM((heads,) + square, f32),
            pltpu.VMEM((heads,) + square, f32),
            pltpu.VMEM((heads, n) + square, bf16),
            DMA((7,)),
            DMA,
            DMA((kinds - units - keys + 2,)),
            DMA((kinds,)),
            DMA,
            DMA((heads,)),
            pltpu.SemaphoreType.REGULAR,
        ]
        + [pltpu.VMEM((n, 2, half, hpg * HEAD_DIM), bf16)] * keys,
        compiler_params=pltpu.CompilerParams(
            collective_id=0, has_side_effects=True, vmem_limit_bytes=48 * 1024 * 1024
        ),
        name="mixer",
    )(*[pltpu.with_memory_space_constraint(x, pltpu.HBM) for x in (table, a_log, dt_bias, qkv, z, gates, conv_weight, gain)])


def per_device(mixed_qkv, gate_z, gate_logits, block_table, conv_weight, a_log, dt_bias, norm_gain):
    n = lax.axis_size("cp")
    segs = lax.axis_size("seg")
    return mixer(
        n, segs, VALUE_HEADS // n, block_table, a_log, dt_bias, mixed_qkv, gate_z, gate_logits.T,
        conv_weight, norm_gain[None, :],
    )


def solution(mesh):
    return jax.shard_map(
        per_device,
        mesh=mesh,
        in_specs=(
            P(("seg", "cp"), None),
            P(("seg", "cp"), None),
            P(("seg", "cp"), None),
            P("seg", None),
            P(),
            P(),
            P(),
            P(),
        ),
        out_specs=P(("seg", "cp"), None),
        check_vma=False,
    )
```

```python
import functools

import jax
import jax.numpy as jnp
from jax import lax
from jax.experimental import pallas as pl
from jax.experimental.pallas import tpu as pltpu
from jax.sharding import PartitionSpec as P

VALUE_HEADS = 32
KEY_HEADS = 16
HEAD_DIM = 128
CONV = 4
BLOCK = 128
TAIL = 8
GROUP = VALUE_HEADS // KEY_HEADS
BATCH = 4

f32 = jnp.float32
bf16 = jnp.bfloat16
MESH = pl.DeviceIdType.MESH

NN = (((1,), (0,)), ((), ()))
NT = (((1,), (1,)), ((), ()))


def split(x):
    hi = x.astype(bf16)
    return hi, (x - hi.astype(f32)).astype(bf16)


def mm(a, b, dims=NN):
    def dot(x, y):
        return lax.dot_general(x, y, dims, preferred_element_type=f32)

    if dims == NT:
        return dot(a[0], b[0]) + (dot(a[0], b[1]) + dot(a[1], b[0]))
    wide = jnp.concatenate(a, axis=1)
    if b[0].shape[1] > HEAD_DIM:
        return dot(wide, jnp.concatenate([b[0], b[0]], axis=0)) + dot(a[0], b[1])
    top = jnp.concatenate([b[0], b[1]], axis=1)
    low = jnp.concatenate([b[0], jnp.zeros_like(b[1])], axis=1)
    both = dot(wide, jnp.concatenate([top, low], axis=0))
    return both[:, :HEAD_DIM] + both[:, HEAD_DIM:]


def log1p_exact(y):
    u = 1.0 + y
    return jnp.where(u == 1.0, y, jnp.log(u) * (y / jnp.where(u == 1.0, 1.0, u - 1.0)))


def scope(name):
    return jax.named_scope(name)


def squares():
    row = lax.broadcasted_iota(jnp.int32, (BLOCK, BLOCK), 0)
    col = lax.broadcasted_iota(jnp.int32, (BLOCK, BLOCK), 1)
    return row, col


def gate_terms(hpg, half_index, g, row_shift, places, gbuf, rate_ref):
    lane = lax.broadcasted_iota(jnp.int32, (8, BLOCK), 1)
    betas, decays = [], []
    for i0, i1 in places:
        one = pltpu.roll(gbuf[i0].astype(f32), (BLOCK // 2) * half_index, 1)
        two = pltpu.roll(gbuf[i1].astype(f32), (BLOCK // 2) * (1 - half_index), 1)
        found = pltpu.roll(jnp.where(lane < BLOCK // 2, one, two), row_shift, 0)
        betas.append(1.0 / (1.0 + jnp.exp(-found)))
        shifted = pltpu.roll(found, 4, 0) + rate_ref[g, 1]
        soft = jnp.maximum(shifted, 0.0) + log1p_exact(jnp.exp(-jnp.abs(shifted)))
        decays.append(rate_ref[g, 0] * soft)
    beta = jnp.concatenate(betas, axis=0)
    decay = jnp.concatenate(decays, axis=0)
    row, col = squares()
    upto = jnp.where(row <= col, 1.0, 0.0).astype(bf16)
    d0 = decay.astype(bf16)
    rest = decay - d0.astype(f32)
    d1 = rest.astype(bf16)
    d2 = (rest - d1.astype(f32)).astype(bf16)
    cum = jnp.dot(d2, upto, preferred_element_type=f32)
    cum = cum + jnp.dot(d1, upto, preferred_element_type=f32)
    cum = cum + jnp.dot(d0, upto, preferred_element_type=f32)
    count = beta.shape[0]
    spare = jnp.zeros((BLOCK - 2 * count, BLOCK), f32)
    turned = jnp.transpose(jnp.concatenate([beta, cum, spare], axis=0))
    return cum, turned, count


def prepare(hpg, blk, g, cum, turned, count, w_ref, x_ref):
    row, col = squares()
    strict = row > col
    inclusive = row >= col

    def conv(start):
        cols = slice(start, start + HEAD_DIM)
        total_rows = w_ref[g, 0:1, cols] * x_ref[5 : 5 + BLOCK, cols]
        for j in range(1, CONV):
            total_rows = total_rows + w_ref[g, j : j + 1, cols] * x_ref[5 + j : 5 + j + BLOCK, cols]
        return total_rows / (1.0 + jnp.exp(-total_rows))

    def unit(x):
        return x * lax.rsqrt(jnp.sum(x * x, axis=-1, keepdims=True) + 1e-06)

    queries = unit(conv(0)) * HEAD_DIM ** (-0.5)
    key_rows = unit(conv(HEAD_DIM))
    ks = split(key_rows)
    qs = split(queries)
    kk = mm(ks, ks, NT)
    qk = mm(qs, ks, NT)
    lower, scores, rhs, kdt, qd, last = [], [], [], [], [], []
    for e in range(hpg):
        at = blk * 8 + e
        beta = turned[:, at : at + 1]
        c = turned[:, count + at : count + at + 1]
        ct = cum[at : at + 1, :]
        final = ct[:, BLOCK - 1 :]
        spread = c - ct
        incl = jnp.where(inclusive, jnp.exp(jnp.where(inclusive, spread, 0.0)), 0.0)
        lower.append(jnp.where(strict, beta * kk * incl, 0.0))
        scores.append(split(qk * incl))
        grow = jnp.exp(c)
        values = conv((2 + e) * HEAD_DIM)
        rhs.append(split(jnp.concatenate([values * beta, key_rows * (beta * grow)], axis=1)))
        kdt.append(split(jnp.transpose(key_rows * jnp.exp(final - c))))
        qd.append(queries * grow)
        last.append(jnp.exp(final))
    return lower, scores, rhs, kdt, qd, last


def blocks(n, hpg, g, half_index, first, row_shift, order, cur, prior, gbuf, rate_ref, w_ref, x_ref, o_ref, mh_ref, ml_ref, st_ref):
    half = cur.shape[1]
    row, col = squares()
    eye = jnp.where(row == col, 1.0, 0.0).astype(f32)
    places = [(order[2 * (first + k)], order[2 * (first + k) + 1]) for k in range(BATCH)]
    cum, turned, count = gate_terms(hpg, half_index, g, row_shift, places, gbuf, rate_ref)
    lower, scores, rhs, kdt, qd, last = [], [], [], [], [], []
    for k in range(BATCH):
        b = first + k
        if k:
            x_ref[k, 0:8, :] = cur[places[k - 1][1], half - 16 :, :].astype(f32)[8:]
        else:
            ahead = order[jnp.maximum(2 * b - 1, 0)]
            near = cur[ahead, half - 16 :, :].astype(f32)[8:]
            x_ref[k, 0:8, :] = jnp.where(lax.rem(b, n // 2) == 0, prior[...], near)
        x_ref[k, 8 : 8 + half, :] = cur[places[k][0]].astype(f32)
        x_ref[k, 8 + half : 8 + 2 * half, :] = cur[places[k][1]].astype(f32)
        found = prepare(hpg, k, g, cum, turned, count, w_ref, x_ref.at[k])
        for total, more in zip((lower, scores, rhs, kdt, qd, last), found):
            total += more
    hs = range(BATCH * hpg)

    def same(size):
        return (row // size) == (col // size)

    small = 16
    power = [split(jnp.where(same(small), -lower[h], 0.0)) for h in hs]
    inverse = [eye + jnp.where(same(small), -lower[h], 0.0) for h in hs]
    steps = 1
    while 2**steps < small:
        power = [split(mm(power[h], power[h])) for h in hs]
        inverse = [inverse[h] + mm(split(inverse[h]), power[h]) for h in hs]
        steps += 1
    size = small
    while size < BLOCK:
        between = same(2 * size) & (~same(size))
        cross = [split(jnp.where(between, lower[h], 0.0)) for h in hs]
        parts = [split(inverse[h]) for h in hs]
        mixed = [split(mm(cross[h], parts[h])) for h in hs]
        inverse = [inverse[h] - mm(parts[h], mixed[h]) for h in hs]
        size *= 2
    solved = [split(mm(split(inverse[h]), rhs[h])) for h in hs]
    outs = [mm(scores[h], solved[h]) for h in hs]
    ends = [mm(kdt[h], solved[h]) for h in hs]
    readers = [split(qd[h] - outs[h][:, HEAD_DIM:]) for h in hs]
    maps = [split(last[h] * eye - ends[h][:, HEAD_DIM:]) for h in hs]
    for k in range(BATCH):
        b = first + k
        states = [split(st_ref[g, e]) for e in range(hpg)]
        for e in range(hpg):
            at = k * hpg + e
            moved = mm(maps[at], states[e])
            st_ref[g, e] = jnp.concatenate(
                [moved[:, :HEAD_DIM] + ends[at][:, :HEAD_DIM], moved[:, HEAD_DIM:]], axis=1
            )
        for e in range(hpg):
            at = k * hpg + e
            seen = mm(readers[at], states[e])
            o_ref[g * hpg + e, b] = seen[:, :HEAD_DIM] + outs[at][:, :HEAD_DIM]
            reach = split(seen[:, HEAD_DIM:])
            mh_ref[g * hpg + e, b] = reach[0]
            ml_ref[g * hpg + e, b] = reach[1]


def whole_kernel(
    n, segs, heads, table_any, a_log_any, dt_bias_any, qkv, z, gates, conv_weight, gain_any, out,
    table, a_log, dt_bias, gain_ref, stage, gstage, gsend, tstage, tsend,
    xin, otail, gbuf, ptab, cur, prior, x_ref, w_ref, rate_ref, order, o_ref, mh_ref, ml_ref, st_ref,
    inc_ref, pass_ref, y_ref, lin, lout, ssem, rsem, hsend, hrecv, ready, *oz
):
    me = lax.axis_index("cp")
    seg = lax.axis_index("seg")
    final = segs - 1
    after = lax.rem(seg + 1, segs)
    before = lax.rem(seg + segs - 1, segs)
    keys = max(1, heads // GROUP)
    hpg = heads // keys
    units = 2 * keys
    key_width = KEY_HEADS * HEAD_DIM
    width = heads * HEAD_DIM
    wz = hpg * HEAD_DIM
    rows = qkv.shape[0]
    half = rows // 2
    AT_TAIL, AT_GATE, AT_Z, AT_TABLE, AT_Y = units, units + keys, units + keys + 1, units + 2 * keys + 1, units + 2 * keys + 2

    barrier = pltpu.get_barrier_semaphore()
    for d in range(1, n):
        pl.semaphore_signal(barrier, inc=1, device_id=(seg, lax.rem(me + d, n)), device_id_type=MESH)

    @pl.when(seg < final)
    def _():
        pl.semaphore_signal(barrier, inc=1, device_id=(after, me), device_id_type=MESH)

    small = [
        pltpu.make_async_copy(src, dst, lin.at[i])
        for i, (src, dst) in enumerate(
            (
                (gates, gstage),
                (qkv.at[pl.ds(rows - TAIL, TAIL)], tstage),
                (table_any, table),
                (a_log_any, a_log),
                (dt_bias_any, dt_bias),
                (gain_any, gain_ref),
            )
        )
    ]
    firsts = sorted({p * heads // GROUP for p in range(n)})
    ahead = [(i * HEAD_DIM, HEAD_DIM) for key in firsts for i in (key, KEY_HEADS + key)]
    ahead += [((2 * KEY_HEADS + p * heads) * HEAD_DIM, wz) for p in range(n)]
    for start, size in ahead:
        pltpu.make_async_copy(qkv.at[pl.ds(0, half), pl.ds(start, size)], stage.at[:, pl.ds(start, size)], lin.at[6]).start()
    for copy in small:
        copy.start()

    def columns(start, size):
        return pl.ds(pl.multiple_of(start, HEAD_DIM), size)

    def places(p, g):
        key = (lax.div(p * heads, GROUP) + g) * HEAD_DIM
        value = (p * heads + g * hpg) * HEAD_DIM
        return (
            (columns(key, HEAD_DIM), pl.ds(0, HEAD_DIM)),
            (columns(key_width + key, HEAD_DIM), pl.ds(HEAD_DIM, HEAD_DIM)),
            (columns(2 * key_width + value, wz), pl.ds(2 * HEAD_DIM, wz)),
        )

    def unit_pieces(p, u, slot):
        if u == 0:
            return [(stage.at[:, src], xin.at[u, slot, :, dst]) for src, dst in places(p, u // 2)]
        return [(qkv.at[pl.ds(u % 2 * half, half), src], xin.at[u, slot, :, dst]) for src, dst in places(p, u // 2)]

    def gate_pieces(p, slot):
        return [(gsend.at[p], gbuf.at[slot])]

    def z_pieces(p, g, slot):
        cols = columns((p * heads + g * hpg) * HEAD_DIM, wz)
        return [(z.at[pl.ds(hf * half, half), cols], oz[g].at[slot, hf]) for hf in range(2)]

    for g in range(keys):
        for src, dst in places(me, g):
            pltpu.make_async_copy(conv_weight.at[:, src], w_ref.at[g, :, dst], lout).start()
    small[0].wait()
    line = lax.broadcasted_iota(jnp.int32, (8, BLOCK), 0)
    for p in range(n):
        tile = p * heads // 8 * 8
        shift = p * heads % 8
        strength = pltpu.roll(gstage[tile : tile + 8].astype(f32), (8 - shift) % 8, 0)
        decay = pltpu.roll(gstage[VALUE_HEADS + tile : VALUE_HEADS + tile + 8].astype(f32), (12 - shift) % 8, 0)
        gsend[p] = jnp.where(line < 4, strength, decay).astype(bf16)
    gbuf[me] = gsend[me]
    staged = stage.at[:, pl.ds(0, sum(size for _, size in ahead))]
    pltpu.make_async_copy(staged, staged, lin.at[6]).wait()
    for kind, found in [(u, unit_pieces(me, u, me)) for u in range(units)] + [
        (AT_Z + g, z_pieces(me, g, me)) for g in range(keys)
    ]:
        for src, dst in found:
            pltpu.make_async_copy(src, dst, rsem.at[kind]).start()
    with scope("entry"):
        pl.semaphore_wait(barrier, n - 1 + jnp.where(seg > 0, 1, 0))

    @pl.when(seg > 0)
    def _():
        pl.semaphore_signal(ready, inc=1, device_id=(before, me), device_id_type=MESH)

    def shared(kind):
        if not isinstance(kind, int):
            return 0
        return 0 if kind < units else 1 if kind < units + keys else kind - units - keys + 2

    def post(kind, src, dst, target):
        pltpu.make_async_remote_copy(
            src_ref=src, dst_ref=dst, send_sem=ssem.at[shared(kind)], recv_sem=rsem.at[kind],
            device_id=target, device_id_type=MESH,
        ).start()

    def remote(kind, ref):
        return pltpu.make_async_remote_copy(
            src_ref=ref, dst_ref=ref, send_sem=ssem.at[shared(kind)], recv_sem=rsem.at[kind],
            device_id=(seg, lax.rem(me + 1, n)), device_id_type=MESH,
        )

    others = pl.ds(0, n - 1)

    def post_all(kind, find):
        for d in range(1, n):
            peer = lax.rem(me + d, n)
            for src, dst in find(peer):
                post(kind, src, dst, (seg, peer))

    post_all(AT_GATE, lambda p: gate_pieces(p, me))
    post_all(0, lambda p: unit_pieces(p, 0, me))
    for copy in small[1:]:
        copy.wait()

    wide = hpg + 2
    pairs = (wide + 1) // 2
    upper = lax.broadcasted_iota(jnp.int32, (TAIL, HEAD_DIM), 0) < TAIL // 2
    for g in range(keys):
        for p in range(n):
            key = p * heads // GROUP + g
            at = [key, KEY_HEADS + key] + [2 * KEY_HEADS + p * heads + g * hpg + e for e in range(hpg)]
            tiles = [tstage[:, i * HEAD_DIM : (i + 1) * HEAD_DIM].astype(f32) for i in at]
            for i in range(pairs):
                low = tiles[i + pairs] if i + pairs < wide else tiles[i]
                both = jnp.where(upper, pltpu.roll(tiles[i], TAIL // 2, 0), low)
                tsend[g, p, :, i * HEAD_DIM : (i + 1) * HEAD_DIM] = both.astype(bf16)

    def find(b, carry):
        parity = lax.div(b, n)
        place = jnp.int32(0)
        for j in range(n):
            place = jnp.where(table[0, 2 * j + parity] == b, j, place)
        order[b] = place
        return carry

    lax.fori_loop(0, 2 * n, find, 0)

    row, col = squares()
    for g in range(keys):
        scale = jnp.zeros((8, BLOCK), f32)
        shift = jnp.zeros((8, BLOCK), f32)
        for e in range(hpg):
            h = me * heads + g * hpg + e
            scale = jnp.where(line == e, a_log[h], scale)
            shift = jnp.where(line == e, dt_bias[h], shift)
            st_ref[g, e, :, :HEAD_DIM] = jnp.zeros((HEAD_DIM, HEAD_DIM), f32)
            st_ref[g, e, :, HEAD_DIM:] = jnp.where(row == col, 1.0, 0.0).astype(f32)
        rate_ref[g, 0] = -jnp.exp(scale)
        rate_ref[g, 1] = shift

    @pl.when(seg < final)
    def _():
        with scope("readywait"):
            pl.semaphore_wait(ready, 1)
        post(AT_TABLE, table_any, ptab, (after, me))
        for g in range(keys):
            for d in range(n):
                peer = lax.rem(me + d, n)
                post(AT_TAIL + g, tsend.at[g, peer], otail.at[g, me], (after, peer))

    for u in range(1, units):
        post_all(u, lambda p: unit_pieces(p, u, me))
    for g in range(keys):
        post_all(AT_Z + g, lambda p: z_pieces(p, g, me))

    pltpu.make_async_copy(w_ref, w_ref, lout).wait()
    with scope("gatewait"):
        remote(AT_GATE, gbuf.at[others]).wait_recv()

    @pl.when(seg > 0)
    def _():
        remote(AT_TABLE, ptab).wait_recv()

    def hop(h):
        return pltpu.make_async_remote_copy(
            src_ref=pass_ref.at[h],
            dst_ref=inc_ref.at[h],
            send_sem=hsend,
            recv_sem=hrecv.at[h],
            device_id=(after, me),
            device_id_type=MESH,
        )

    def forward(g):
        @pl.when((seg == 0) & (seg < final))
        def _():
            for e in range(hpg):
                h = g * hpg + e
                pass_ref[h] = st_ref[g, e, :, :HEAD_DIM]
                hop(h).start()

        @pl.when((seg > 0) & (seg < final))
        def _():
            for e in range(hpg):
                h = g * hpg + e
                through = split(st_ref[g, e, :, HEAD_DIM:])
                with scope("hopmid"):
                    hop(h).wait_recv()
                pass_ref[h] = st_ref[g, e, :, :HEAD_DIM] + mm(through, split(inc_ref[h]))
                hop(h).start()

    def one_unit(u, carry):
        g = lax.div(u, 2)
        half_index = lax.rem(u, 2)
        with scope("unitwait"):
            remote(u, xin.at[u]).wait_recv()

        @pl.when((half_index == 0) & (seg == 0))
        def _():
            prior[...] = jnp.zeros_like(prior)

        @pl.when((half_index == 0) & (seg > 0))
        def _():
            with scope("tailwait"):
                remote(AT_TAIL + g, otail.at[g]).wait_recv()
            found = jnp.zeros(otail.shape[2:], f32)
            for j in range(n):
                hit = ptab[0:1, 2 * j + 1 : 2 * j + 2] == 2 * n - 1
                found = jnp.where(hit, otail[g, j].astype(f32), found)
            for i in range(wide):
                pair = found[:, i % pairs * HEAD_DIM : (i % pairs + 1) * HEAD_DIM]
                prior[:, i * HEAD_DIM : (i + 1) * HEAD_DIM] = pltpu.roll(pair, TAIL // 2, 0) if i < pairs else pair

        @pl.when(half_index == 1)
        def _():
            prior[...] = cur[order[n - 1], half - 16 :, :].astype(f32)[8:]

        cur[...] = xin[u]
        row_shift = lax.rem(8 - g * hpg, 8)

        def batch(first):
            blocks(
                n, hpg, g, half_index, first, row_shift, order, cur, prior, gbuf, rate_ref,
                w_ref, x_ref, o_ref, mh_ref, ml_ref, st_ref,
            )

        turns = n // 2 // BATCH
        with scope("run"):
            if turns == 1:
                batch(half_index * (n // 2))
            else:
                lax.fori_loop(0, turns, lambda t, c: (batch(half_index * (n // 2) + t * BATCH), c)[1], 0)
        for earlier in range(keys - 1):
            @pl.when(u == jnp.minimum(2 * earlier + 1 + seg, units - 1))
            def _():
                forward(earlier)
        return carry

    lax.fori_loop(0, units, one_unit, 0)

    def block(h, b, state):
        g, e = h // hpg, h % hpg
        i0 = order[2 * b]
        i1 = order[2 * b + 1]
        which = lax.div(b, n // 2)
        cols = pl.ds(e * HEAD_DIM, HEAD_DIM)
        core = o_ref[h, b] + mm((mh_ref[h, b], ml_ref[h, b]), state)
        gate = jnp.concatenate([oz[g][i0, which, :, cols], oz[g][i1, which, :, cols]], axis=0).astype(f32)
        scale = lax.rsqrt(jnp.sum(core * core, axis=-1, keepdims=True) * (1.0 / HEAD_DIM) + 1e-06)
        y_ref[h, b] = (core * scale * gain_ref[0:1, :] * (gate / (1.0 + jnp.exp(-gate)))).astype(bf16)

    def target(h, source):
        return out.at[:, columns(source * width + h * HEAD_DIM, HEAD_DIM)]

    def give(h, d):
        peer = lax.rem(me + d, n)
        post(AT_Y, y_ref.at[h, peer], target(h, me), (seg, peer))

    def close(h):
        @pl.when(seg == 0)
        def _():
            inc_ref[h] = jnp.zeros((HEAD_DIM, HEAD_DIM), f32)

        @pl.when((seg == final) & (seg > 0))
        def _():
            with scope("hoplast"):
                hop(h).wait_recv()

        state = split(inc_ref[h])
        for d in range(1, n):
            block(h, lax.rem(me + d, n), state)
            if d > 1:
                give(h, d - 1)
        block(h, me, state)
        give(h, n - 1)
        pltpu.make_async_copy(y_ref.at[h, me], target(h, me), rsem.at[AT_Y]).start()

    for h in range(heads):
        g = h // hpg
        late = heads - hpg
        for turn in range(late + 1):
            if h == turn:
                with scope("forward"):
                    pl.when(jnp.minimum(seg, late) == turn)(lambda: forward(keys - 1))
        if h % hpg == 0:
            with scope("zwait"):
                remote(AT_Z + g, oz[g]).wait_recv()
        with scope("close"):
            close(h)

    with scope("waity"):
        remote(AT_Y, y_ref).wait_recv()
    with scope("drain"):
        remote(AT_GATE, gbuf.at[others]).wait_send()
        remote(0, xin.at[:, others]).wait_send()
        for g in range(keys):
            remote(AT_Z + g, oz[g].at[others]).wait_send()
        remote(AT_Y, y_ref.at[:, others]).wait_send()

        @pl.when(seg < final)
        def _():
            remote(AT_TABLE, ptab).wait_send()
            remote(AT_TAIL, otail).wait_send()
            pltpu.make_async_remote_copy(
                src_ref=pass_ref, dst_ref=inc_ref, send_sem=hsend, recv_sem=hrecv.at[0],
                device_id=(after, me), device_id_type=MESH,
            ).wait_send()


def mixer(n, segs, heads, table, a_log, dt_bias, qkv, z, gates, conv_weight, gain):
    keys = max(1, heads // GROUP)
    hpg = heads // keys
    units = 2 * keys
    half = qkv.shape[0] // 2
    wide = (2 + hpg) * HEAD_DIM
    packed = (3 + hpg) // 2 * HEAD_DIM
    anywhere = pl.BlockSpec(memory_space=pl.ANY)
    vmem = pl.BlockSpec(memory_space=pltpu.VMEM)
    square = (HEAD_DIM, HEAD_DIM)
    DMA = pltpu.SemaphoreType.DMA
    kinds = units + 2 * keys + 3
    return pl.pallas_call(
        functools.partial(whole_kernel, n, segs, heads),
        out_shape=pltpu.VMEM((BLOCK, n * heads * HEAD_DIM), bf16),
        in_specs=[anywhere] * 8,
        out_specs=vmem,
        scratch_shapes=[
            pltpu.SMEM(table.shape, jnp.int32),
            pltpu.SMEM(a_log.shape, f32),
            pltpu.SMEM(dt_bias.shape, f32),
            pltpu.VMEM(gain.shape, f32),
            pltpu.VMEM((half, qkv.shape[1]), bf16),
            pltpu.VMEM(gates.shape, bf16),
            pltpu.VMEM((n, 8, BLOCK), bf16),
            pltpu.VMEM((TAIL, qkv.shape[1]), bf16),
            pltpu.VMEM((keys, n, TAIL, packed), bf16),
            pltpu.VMEM((units, n, half, wide), bf16),
            pltpu.VMEM((keys, n, TAIL, packed), bf16),
            pltpu.VMEM((n, 8, BLOCK), bf16),
            pltpu.VMEM(table.shape, jnp.int32),
            pltpu.VMEM((n, half, wide), bf16),
            pltpu.VMEM((TAIL, wide), f32),
            pltpu.VMEM((BATCH, BLOCK + 8, wide), f32),
            pltpu.VMEM((keys, CONV, wide), f32),
            pltpu.VMEM((keys, 2, 8, BLOCK), f32),
            pltpu.SMEM((2 * n,), jnp.int32),
            pltpu.VMEM((heads, n) + square, f32),
            pltpu.VMEM((heads, n) + square, bf16),
            pltpu.VMEM((heads, n) + square, bf16),
            pltpu.VMEM((keys, hpg, HEAD_DIM, 2 * HEAD_DIM), f32),
            pltpu.VMEM((heads,) + square, f32),
            pltpu.VMEM((heads,) + square, f32),
            pltpu.VMEM((heads, n) + square, bf16),
            DMA((7,)),
            DMA,
            DMA((kinds - units - keys + 2,)),
            DMA((kinds,)),
            DMA,
            DMA((heads,)),
            pltpu.SemaphoreType.REGULAR,
        ]
        + [pltpu.VMEM((n, 2, half, hpg * HEAD_DIM), bf16)] * keys,
        compiler_params=pltpu.CompilerParams(
            collective_id=0, has_side_effects=True, vmem_limit_bytes=48 * 1024 * 1024
        ),
        name="mixer",
    )(*[pltpu.with_memory_space_constraint(x, pltpu.HBM) for x in (table, a_log, dt_bias, qkv, z, gates, conv_weight, gain)])


def per_device(mixed_qkv, gate_z, gate_logits, block_table, conv_weight, a_log, dt_bias, norm_gain):
    n = lax.axis_size("cp")
    segs = lax.axis_size("seg")
    return mixer(
        n, segs, VALUE_HEADS // n, block_table, a_log, dt_bias, mixed_qkv, gate_z, gate_logits.T,
        conv_weight, norm_gain[None, :],
    )


def solution(mesh):
    return jax.shard_map(
        per_device,
        mesh=mesh,
        in_specs=(
            P(("seg", "cp"), None),
            P(("seg", "cp"), None),
            P(("seg", "cp"), None),
            P("seg", None),
            P(),
            P(),
            P(),
            P(),
        ),
        out_specs=P(("seg", "cp"), None),
        check_vma=False,
    )
```

```python
import functools

import jax
import jax.numpy as jnp
from jax import lax
from jax.experimental import pallas as pl
from jax.experimental.pallas import tpu as pltpu
from jax.sharding import PartitionSpec as P

VALUE_HEADS = 32
KEY_HEADS = 16
HEAD_DIM = 128
CONV = 4
BLOCK = 128
TAIL = 8
GROUP = VALUE_HEADS // KEY_HEADS
BATCH = 4

f32 = jnp.float32
bf16 = jnp.bfloat16
MESH = pl.DeviceIdType.MESH

NN = (((1,), (0,)), ((), ()))
NT = (((1,), (1,)), ((), ()))


def split(x):
    hi = x.astype(bf16)
    return hi, (x - hi.astype(f32)).astype(bf16)


def mm(a, b, dims=NN):
    def dot(x, y):
        return lax.dot_general(x, y, dims, preferred_element_type=f32)

    if dims == NT:
        return dot(a[0], b[0]) + (dot(a[0], b[1]) + dot(a[1], b[0]))
    wide = jnp.concatenate(a, axis=1)
    if b[0].shape[1] > HEAD_DIM:
        return dot(wide, jnp.concatenate([b[0], b[0]], axis=0)) + dot(a[0], b[1])
    top = jnp.concatenate([b[0], b[1]], axis=1)
    low = jnp.concatenate([b[0], jnp.zeros_like(b[1])], axis=1)
    both = dot(wide, jnp.concatenate([top, low], axis=0))
    return both[:, :HEAD_DIM] + both[:, HEAD_DIM:]


def log1p_exact(y):
    u = 1.0 + y
    return jnp.where(u == 1.0, y, jnp.log(u) * (y / jnp.where(u == 1.0, 1.0, u - 1.0)))


def scope(name):
    return jax.named_scope(name)


def squares():
    row = lax.broadcasted_iota(jnp.int32, (BLOCK, BLOCK), 0)
    col = lax.broadcasted_iota(jnp.int32, (BLOCK, BLOCK), 1)
    return row, col


def gate_terms(hpg, half_index, g, row_shift, places, gbuf, rate_ref):
    lane = lax.broadcasted_iota(jnp.int32, (8, BLOCK), 1)
    betas, decays = [], []
    for i0, i1 in places:
        one = pltpu.roll(gbuf[i0].astype(f32), (BLOCK // 2) * half_index, 1)
        two = pltpu.roll(gbuf[i1].astype(f32), (BLOCK // 2) * (1 - half_index), 1)
        found = pltpu.roll(jnp.where(lane < BLOCK // 2, one, two), row_shift, 0)
        betas.append(1.0 / (1.0 + jnp.exp(-found)))
        shifted = pltpu.roll(found, 4, 0) + rate_ref[g, 1]
        soft = jnp.maximum(shifted, 0.0) + log1p_exact(jnp.exp(-jnp.abs(shifted)))
        decays.append(rate_ref[g, 0] * soft)
    beta = jnp.concatenate(betas, axis=0)
    decay = jnp.concatenate(decays, axis=0)
    row, col = squares()
    upto = jnp.where(row <= col, 1.0, 0.0).astype(bf16)
    d0 = decay.astype(bf16)
    rest = decay - d0.astype(f32)
    d1 = rest.astype(bf16)
    d2 = (rest - d1.astype(f32)).astype(bf16)
    cum = jnp.dot(d2, upto, preferred_element_type=f32)
    cum = cum + jnp.dot(d1, upto, preferred_element_type=f32)
    cum = cum + jnp.dot(d0, upto, preferred_element_type=f32)
    count = beta.shape[0]
    spare = jnp.zeros((BLOCK - 2 * count, BLOCK), f32)
    turned = jnp.transpose(jnp.concatenate([beta, cum, spare], axis=0))
    return cum, turned, count


def prepare(hpg, blk, g, cum, turned, count, w_ref, x_ref):
    row, col = squares()
    strict = row > col
    inclusive = row >= col

    def conv(start):
        cols = slice(start, start + HEAD_DIM)
        total_rows = w_ref[g, 0:1, cols] * x_ref[5 : 5 + BLOCK, cols]
        for j in range(1, CONV):
            total_rows = total_rows + w_ref[g, j : j + 1, cols] * x_ref[5 + j : 5 + j + BLOCK, cols]
        return total_rows / (1.0 + jnp.exp(-total_rows))

    def unit(x):
        return x * lax.rsqrt(jnp.sum(x * x, axis=-1, keepdims=True) + 1e-06)

    queries = unit(conv(0)) * HEAD_DIM ** (-0.5)
    key_rows = unit(conv(HEAD_DIM))
    ks = split(key_rows)
    qs = split(queries)
    kk = mm(ks, ks, NT)
    qk = mm(qs, ks, NT)
    lower, scores, rhs, kdt, qd, last = [], [], [], [], [], []
    for e in range(hpg):
        at = blk * 8 + e
        beta = turned[:, at : at + 1]
        c = turned[:, count + at : count + at + 1]
        ct = cum[at : at + 1, :]
        final = ct[:, BLOCK - 1 :]
        spread = c - ct
        incl = jnp.where(inclusive, jnp.exp(jnp.where(inclusive, spread, 0.0)), 0.0)
        lower.append(jnp.where(strict, beta * kk * incl, 0.0))
        scores.append(split(qk * incl))
        grow = jnp.exp(c)
        values = conv((2 + e) * HEAD_DIM)
        rhs.append(split(jnp.concatenate([values * beta, key_rows * (beta * grow)], axis=1)))
        kdt.append(split(jnp.transpose(key_rows * jnp.exp(final - c))))
        qd.append(queries * grow)
        last.append(jnp.exp(final))
    return lower, scores, rhs, kdt, qd, last


def blocks(n, hpg, g, half_index, first, row_shift, order, cur, prior, gbuf, rate_ref, w_ref, x_ref, o_ref, mh_ref, ml_ref, st_ref):
    half = cur.shape[1]
    row, col = squares()
    eye = jnp.where(row == col, 1.0, 0.0).astype(f32)
    places = [(order[2 * (first + k)], order[2 * (first + k) + 1]) for k in range(BATCH)]
    cum, turned, count = gate_terms(hpg, half_index, g, row_shift, places, gbuf, rate_ref)
    lower, scores, rhs, kdt, qd, last = [], [], [], [], [], []
    for k in range(BATCH):
        b = first + k
        if k:
            x_ref[k, 0:8, :] = cur[places[k - 1][1], half - 16 :, :].astype(f32)[8:]
        else:
            ahead = order[jnp.maximum(2 * b - 1, 0)]
            near = cur[ahead, half - 16 :, :].astype(f32)[8:]
            x_ref[k, 0:8, :] = jnp.where(lax.rem(b, n // 2) == 0, prior[...], near)
        x_ref[k, 8 : 8 + half, :] = cur[places[k][0]].astype(f32)
        x_ref[k, 8 + half : 8 + 2 * half, :] = cur[places[k][1]].astype(f32)
        found = prepare(hpg, k, g, cum, turned, count, w_ref, x_ref.at[k])
        for total, more in zip((lower, scores, rhs, kdt, qd, last), found):
            total += more
    hs = range(BATCH * hpg)

    def same(size):
        return (row // size) == (col // size)

    small = 16
    power = [split(jnp.where(same(small), -lower[h], 0.0)) for h in hs]
    inverse = [eye + jnp.where(same(small), -lower[h], 0.0) for h in hs]
    steps = 1
    while 2**steps < small:
        power = [split(mm(power[h], power[h])) for h in hs]
        inverse = [inverse[h] + mm(split(inverse[h]), power[h]) for h in hs]
        steps += 1
    size = small
    while size < BLOCK:
        between = same(2 * size) & (~same(size))
        cross = [split(jnp.where(between, lower[h], 0.0)) for h in hs]
        parts = [split(inverse[h]) for h in hs]
        mixed = [split(mm(cross[h], parts[h])) for h in hs]
        inverse = [inverse[h] - mm(parts[h], mixed[h]) for h in hs]
        size *= 2
    solved = [split(mm(split(inverse[h]), rhs[h])) for h in hs]
    outs = [mm(scores[h], solved[h]) for h in hs]
    ends = [mm(kdt[h], solved[h]) for h in hs]
    readers = [split(qd[h] - outs[h][:, HEAD_DIM:]) for h in hs]
    maps = [split(last[h] * eye - ends[h][:, HEAD_DIM:]) for h in hs]
    for k in range(BATCH):
        b = first + k
        states = [split(st_ref[g, e]) for e in range(hpg)]
        for e in range(hpg):
            at = k * hpg + e
            moved = mm(maps[at], states[e])
            st_ref[g, e] = jnp.concatenate(
                [moved[:, :HEAD_DIM] + ends[at][:, :HEAD_DIM], moved[:, HEAD_DIM:]], axis=1
            )
        for e in range(hpg):
            at = k * hpg + e
            seen = mm(readers[at], states[e])
            o_ref[g * hpg + e, b] = seen[:, :HEAD_DIM] + outs[at][:, :HEAD_DIM]
            reach = split(seen[:, HEAD_DIM:])
            mh_ref[g * hpg + e, b] = reach[0]
            ml_ref[g * hpg + e, b] = reach[1]


def whole_kernel(
    n, segs, heads, table_any, a_log_any, dt_bias_any, qkv, z, gates, conv_weight, gain_any, out,
    table, a_log, dt_bias, gain_ref, stage, gstage, gsend, tstage, tsend,
    xin, otail, gbuf, ptab, cur, prior, x_ref, w_ref, rate_ref, order, o_ref, mh_ref, ml_ref, st_ref,
    inc_ref, pass_ref, y_ref, lin, lout, ssem, rsem, hsend, hrecv, ready, *oz
):
    me = lax.axis_index("cp")
    seg = lax.axis_index("seg")
    final = segs - 1
    after = lax.rem(seg + 1, segs)
    before = lax.rem(seg + segs - 1, segs)
    keys = max(1, heads // GROUP)
    hpg = heads // keys
    units = 2 * keys
    key_width = KEY_HEADS * HEAD_DIM
    width = heads * HEAD_DIM
    wz = hpg * HEAD_DIM
    rows = qkv.shape[0]
    half = rows // 2
    AT_TAIL, AT_GATE, AT_Z, AT_TABLE, AT_Y = units, units + keys, units + keys + 1, units + 2 * keys + 1, units + 2 * keys + 2

    barrier = pltpu.get_barrier_semaphore()
    for d in range(1, n):
        pl.semaphore_signal(barrier, inc=1, device_id=(seg, lax.rem(me + d, n)), device_id_type=MESH)

    @pl.when(seg < final)
    def _():
        pl.semaphore_signal(barrier, inc=1, device_id=(after, me), device_id_type=MESH)

    small = [
        pltpu.make_async_copy(src, dst, lin.at[i])
        for i, (src, dst) in enumerate(
            (
                (gates, gstage),
                (qkv.at[pl.ds(rows - TAIL, TAIL)], tstage),
                (table_any, table),
                (a_log_any, a_log),
                (dt_bias_any, dt_bias),
                (gain_any, gain_ref),
            )
        )
    ]
    firsts = sorted({p * heads // GROUP for p in range(n)})
    ahead = [(i * HEAD_DIM, HEAD_DIM) for key in firsts for i in (key, KEY_HEADS + key)]
    ahead += [((2 * KEY_HEADS + p * heads) * HEAD_DIM, wz) for p in range(n)]
    for start, size in ahead:
        pltpu.make_async_copy(qkv.at[pl.ds(0, half), pl.ds(start, size)], stage.at[:, pl.ds(start, size)], lin.at[6]).start()
    for copy in small:
        copy.start()

    def columns(start, size):
        return pl.ds(pl.multiple_of(start, HEAD_DIM), size)

    def places(p, g):
        key = (lax.div(p * heads, GROUP) + g) * HEAD_DIM
        value = (p * heads + g * hpg) * HEAD_DIM
        return (
            (columns(key, HEAD_DIM), pl.ds(0, HEAD_DIM)),
            (columns(key_width + key, HEAD_DIM), pl.ds(HEAD_DIM, HEAD_DIM)),
            (columns(2 * key_width + value, wz), pl.ds(2 * HEAD_DIM, wz)),
        )

    def unit_pieces(p, u, slot):
        if u == 0:
            return [(stage.at[:, src], xin.at[u, slot, :, dst]) for src, dst in places(p, u // 2)]
        return [(qkv.at[pl.ds(u % 2 * half, half), src], xin.at[u, slot, :, dst]) for src, dst in places(p, u // 2)]

    def gate_pieces(p, slot):
        return [(gsend.at[p], gbuf.at[slot])]

    def z_pieces(p, g, slot):
        cols = columns((p * heads + g * hpg) * HEAD_DIM, wz)
        return [(z.at[pl.ds(hf * half, half), cols], oz[g].at[slot, hf]) for hf in range(2)]

    for g in range(keys):
        for src, dst in places(me, g):
            pltpu.make_async_copy(conv_weight.at[:, src], w_ref.at[g, :, dst], lout).start()
    small[0].wait()
    line = lax.broadcasted_iota(jnp.int32, (8, BLOCK), 0)
    for p in range(n):
        tile = p * heads // 8 * 8
        shift = p * heads % 8
        strength = pltpu.roll(gstage[tile : tile + 8].astype(f32), (8 - shift) % 8, 0)
        decay = pltpu.roll(gstage[VALUE_HEADS + tile : VALUE_HEADS + tile + 8].astype(f32), (12 - shift) % 8, 0)
        gsend[p] = jnp.where(line < 4, strength, decay).astype(bf16)
    gbuf[me] = gsend[me]
    staged = stage.at[:, pl.ds(0, sum(size for _, size in ahead))]
    pltpu.make_async_copy(staged, staged, lin.at[6]).wait()
    for kind, found in [(u, unit_pieces(me, u, me)) for u in range(units)] + [
        (AT_Z + g, z_pieces(me, g, me)) for g in range(keys)
    ]:
        for src, dst in found:
            pltpu.make_async_copy(src, dst, rsem.at[kind]).start()
    with scope("entry"):
        pl.semaphore_wait(barrier, n - 1 + jnp.where(seg > 0, 1, 0))

    @pl.when(seg > 0)
    def _():
        pl.semaphore_signal(ready, inc=1, device_id=(before, me), device_id_type=MESH)

    def shared(kind):
        if not isinstance(kind, int):
            return 0
        return 0 if kind < units else 1 if kind < units + keys else kind - units - keys + 2

    def post(kind, src, dst, target):
        pltpu.make_async_remote_copy(
            src_ref=src, dst_ref=dst, send_sem=ssem.at[shared(kind)], recv_sem=rsem.at[kind],
            device_id=target, device_id_type=MESH,
        ).start()

    def remote(kind, ref):
        return pltpu.make_async_remote_copy(
            src_ref=ref, dst_ref=ref, send_sem=ssem.at[shared(kind)], recv_sem=rsem.at[kind],
            device_id=(seg, lax.rem(me + 1, n)), device_id_type=MESH,
        )

    others = pl.ds(0, n - 1)

    def post_all(kind, find):
        for d in range(1, n):
            peer = lax.rem(me + d, n)
            for src, dst in find(peer):
                post(kind, src, dst, (seg, peer))

    post_all(AT_GATE, lambda p: gate_pieces(p, me))
    post_all(0, lambda p: unit_pieces(p, 0, me))
    for copy in small[1:]:
        copy.wait()

    wide = hpg + 2
    pairs = (wide + 1) // 2
    upper = lax.broadcasted_iota(jnp.int32, (TAIL, HEAD_DIM), 0) < TAIL // 2
    for g in range(keys):
        for p in range(n):
            key = p * heads // GROUP + g
            at = [key, KEY_HEADS + key] + [2 * KEY_HEADS + p * heads + g * hpg + e for e in range(hpg)]
            tiles = [tstage[:, i * HEAD_DIM : (i + 1) * HEAD_DIM].astype(f32) for i in at]
            for i in range(pairs):
                low = tiles[i + pairs] if i + pairs < wide else tiles[i]
                both = jnp.where(upper, pltpu.roll(tiles[i], TAIL // 2, 0), low)
                tsend[g, p, :, i * HEAD_DIM : (i + 1) * HEAD_DIM] = both.astype(bf16)

    def find(b, carry):
        parity = lax.div(b, n)
        place = jnp.int32(0)
        for j in range(n):
            place = jnp.where(table[0, 2 * j + parity] == b, j, place)
        order[b] = place
        return carry

    lax.fori_loop(0, 2 * n, find, 0)

    row, col = squares()
    for g in range(keys):
        scale = jnp.zeros((8, BLOCK), f32)
        shift = jnp.zeros((8, BLOCK), f32)
        for e in range(hpg):
            h = me * heads + g * hpg + e
            scale = jnp.where(line == e, a_log[h], scale)
            shift = jnp.where(line == e, dt_bias[h], shift)
            st_ref[g, e, :, :HEAD_DIM] = jnp.zeros((HEAD_DIM, HEAD_DIM), f32)
            st_ref[g, e, :, HEAD_DIM:] = jnp.where(row == col, 1.0, 0.0).astype(f32)
        rate_ref[g, 0] = -jnp.exp(scale)
        rate_ref[g, 1] = shift

    def post_tails(g):
        for d in range(n):
            peer = lax.rem(me + d, n)
            post(AT_TAIL + g, tsend.at[g, peer], otail.at[g, me], (after, peer))

    @pl.when(seg < final)
    def _():
        with scope("readywait"):
            pl.semaphore_wait(ready, 1)
        post(AT_TABLE, table_any, ptab, (after, me))
        post_tails(0)

    for u in range(1, units):
        if u % 2 == 0:
            pl.when(seg < final)(functools.partial(post_tails, u // 2))
        post_all(u, lambda p: unit_pieces(p, u, me))
    for g in range(keys):
        post_all(AT_Z + g, lambda p: z_pieces(p, g, me))

    pltpu.make_async_copy(w_ref, w_ref, lout).wait()
    with scope("gatewait"):
        remote(AT_GATE, gbuf.at[others]).wait_recv()

    @pl.when(seg > 0)
    def _():
        remote(AT_TABLE, ptab).wait_recv()

    def hop(h):
        return pltpu.make_async_remote_copy(
            src_ref=pass_ref.at[h],
            dst_ref=inc_ref.at[h],
            send_sem=hsend,
            recv_sem=hrecv.at[h],
            device_id=(after, me),
            device_id_type=MESH,
        )

    def forward(g):
        @pl.when((seg == 0) & (seg < final))
        def _():
            for e in range(hpg):
                h = g * hpg + e
                pass_ref[h] = st_ref[g, e, :, :HEAD_DIM]
                hop(h).start()

        @pl.when((seg > 0) & (seg < final))
        def _():
            for e in range(hpg):
                h = g * hpg + e
                through = split(st_ref[g, e, :, HEAD_DIM:])
                with scope("hopmid"):
                    hop(h).wait_recv()
                pass_ref[h] = st_ref[g, e, :, :HEAD_DIM] + mm(through, split(inc_ref[h]))
                hop(h).start()

    def one_unit(u, carry):
        g = lax.div(u, 2)
        half_index = lax.rem(u, 2)
        with scope("unitwait"):
            remote(u, xin.at[u]).wait_recv()

        @pl.when((half_index == 0) & (seg == 0))
        def _():
            prior[...] = jnp.zeros_like(prior)

        @pl.when((half_index == 0) & (seg > 0))
        def _():
            with scope("tailwait"):
                remote(AT_TAIL + g, otail.at[g]).wait_recv()
            found = jnp.zeros(otail.shape[2:], f32)
            for j in range(n):
                hit = ptab[0:1, 2 * j + 1 : 2 * j + 2] == 2 * n - 1
                found = jnp.where(hit, otail[g, j].astype(f32), found)
            for i in range(wide):
                pair = found[:, i % pairs * HEAD_DIM : (i % pairs + 1) * HEAD_DIM]
                prior[:, i * HEAD_DIM : (i + 1) * HEAD_DIM] = pltpu.roll(pair, TAIL // 2, 0) if i < pairs else pair

        @pl.when(half_index == 1)
        def _():
            prior[...] = cur[order[n - 1], half - 16 :, :].astype(f32)[8:]

        cur[...] = xin[u]
        row_shift = lax.rem(8 - g * hpg, 8)

        def batch(first):
            blocks(
                n, hpg, g, half_index, first, row_shift, order, cur, prior, gbuf, rate_ref,
                w_ref, x_ref, o_ref, mh_ref, ml_ref, st_ref,
            )

        turns = n // 2 // BATCH
        with scope("run"):
            if turns == 1:
                batch(half_index * (n // 2))
            else:
                lax.fori_loop(0, turns, lambda t, c: (batch(half_index * (n // 2) + t * BATCH), c)[1], 0)
        for earlier in range(keys - 1):
            @pl.when(u == jnp.minimum(2 * earlier + 1 + seg, units - 1))
            def _():
                forward(earlier)
        return carry

    lax.fori_loop(0, units, one_unit, 0)

    def block(h, b, state):
        g, e = h // hpg, h % hpg
        i0 = order[2 * b]
        i1 = order[2 * b + 1]
        which = lax.div(b, n // 2)
        cols = pl.ds(e * HEAD_DIM, HEAD_DIM)
        core = o_ref[h, b] + mm((mh_ref[h, b], ml_ref[h, b]), state)
        gate = jnp.concatenate([oz[g][i0, which, :, cols], oz[g][i1, which, :, cols]], axis=0).astype(f32)
        scale = lax.rsqrt(jnp.sum(core * core, axis=-1, keepdims=True) * (1.0 / HEAD_DIM) + 1e-06)
        y_ref[h, b] = (core * scale * gain_ref[0:1, :] * (gate / (1.0 + jnp.exp(-gate)))).astype(bf16)

    def target(h, source):
        return out.at[:, columns(source * width + h * HEAD_DIM, HEAD_DIM)]

    def give(h, d):
        peer = lax.rem(me + d, n)
        post(AT_Y, y_ref.at[h, peer], target(h, me), (seg, peer))

    def close(h):
        @pl.when(seg == 0)
        def _():
            inc_ref[h] = jnp.zeros((HEAD_DIM, HEAD_DIM), f32)

        @pl.when((seg == final) & (seg > 0))
        def _():
            with scope("hoplast"):
                hop(h).wait_recv()

        state = split(inc_ref[h])
        for d in range(1, n):
            block(h, lax.rem(me + d, n), state)
            if d > 1:
                give(h, d - 1)
        block(h, me, state)
        give(h, n - 1)
        pltpu.make_async_copy(y_ref.at[h, me], target(h, me), rsem.at[AT_Y]).start()

    for h in range(heads):
        g = h // hpg
        late = heads - hpg
        for turn in range(late + 1):
            if h == turn:
                with scope("forward"):
                    pl.when(jnp.minimum(seg, late) == turn)(lambda: forward(keys - 1))
        if h % hpg == 0:
            with scope("zwait"):
                remote(AT_Z + g, oz[g]).wait_recv()
        with scope("close"):
            close(h)

    with scope("waity"):
        remote(AT_Y, y_ref).wait_recv()
    with scope("drain"):
        remote(AT_GATE, gbuf.at[others]).wait_send()
        remote(0, xin.at[:, others]).wait_send()
        for g in range(keys):
            remote(AT_Z + g, oz[g].at[others]).wait_send()
        remote(AT_Y, y_ref.at[:, others]).wait_send()

        @pl.when(seg < final)
        def _():
            remote(AT_TABLE, ptab).wait_send()
            remote(AT_TAIL, otail).wait_send()
            pltpu.make_async_remote_copy(
                src_ref=pass_ref, dst_ref=inc_ref, send_sem=hsend, recv_sem=hrecv.at[0],
                device_id=(after, me), device_id_type=MESH,
            ).wait_send()


def mixer(n, segs, heads, table, a_log, dt_bias, qkv, z, gates, conv_weight, gain):
    keys = max(1, heads // GROUP)
    hpg = heads // keys
    units = 2 * keys
    half = qkv.shape[0] // 2
    wide = (2 + hpg) * HEAD_DIM
    packed = (3 + hpg) // 2 * HEAD_DIM
    anywhere = pl.BlockSpec(memory_space=pl.ANY)
    vmem = pl.BlockSpec(memory_space=pltpu.VMEM)
    square = (HEAD_DIM, HEAD_DIM)
    DMA = pltpu.SemaphoreType.DMA
    kinds = units + 2 * keys + 3
    return pl.pallas_call(
        functools.partial(whole_kernel, n, segs, heads),
        out_shape=pltpu.VMEM((BLOCK, n * heads * HEAD_DIM), bf16),
        in_specs=[anywhere] * 8,
        out_specs=vmem,
        scratch_shapes=[
            pltpu.SMEM(table.shape, jnp.int32),
            pltpu.SMEM(a_log.shape, f32),
            pltpu.SMEM(dt_bias.shape, f32),
            pltpu.VMEM(gain.shape, f32),
            pltpu.VMEM((half, qkv.shape[1]), bf16),
            pltpu.VMEM(gates.shape, bf16),
            pltpu.VMEM((n, 8, BLOCK), bf16),
            pltpu.VMEM((TAIL, qkv.shape[1]), bf16),
            pltpu.VMEM((keys, n, TAIL, packed), bf16),
            pltpu.VMEM((units, n, half, wide), bf16),
            pltpu.VMEM((keys, n, TAIL, packed), bf16),
            pltpu.VMEM((n, 8, BLOCK), bf16),
            pltpu.VMEM(table.shape, jnp.int32),
            pltpu.VMEM((n, half, wide), bf16),
            pltpu.VMEM((TAIL, wide), f32),
            pltpu.VMEM((BATCH, BLOCK + 8, wide), f32),
            pltpu.VMEM((keys, CONV, wide), f32),
            pltpu.VMEM((keys, 2, 8, BLOCK), f32),
            pltpu.SMEM((2 * n,), jnp.int32),
            pltpu.VMEM((heads, n) + square, f32),
            pltpu.VMEM((heads, n) + square, bf16),
            pltpu.VMEM((heads, n) + square, bf16),
            pltpu.VMEM((keys, hpg, HEAD_DIM, 2 * HEAD_DIM), f32),
            pltpu.VMEM((heads,) + square, f32),
            pltpu.VMEM((heads,) + square, f32),
            pltpu.VMEM((heads, n) + square, bf16),
            DMA((7,)),
            DMA,
            DMA((kinds - units - keys + 2,)),
            DMA((kinds,)),
            DMA,
            DMA((heads,)),
            pltpu.SemaphoreType.REGULAR,
        ]
        + [pltpu.VMEM((n, 2, half, hpg * HEAD_DIM), bf16)] * keys,
        compiler_params=pltpu.CompilerParams(
            collective_id=0, has_side_effects=True, vmem_limit_bytes=48 * 1024 * 1024
        ),
        name="mixer",
    )(*[pltpu.with_memory_space_constraint(x, pltpu.HBM) for x in (table, a_log, dt_bias, qkv, z, gates, conv_weight, gain)])


def per_device(mixed_qkv, gate_z, gate_logits, block_table, conv_weight, a_log, dt_bias, norm_gain):
    n = lax.axis_size("cp")
    segs = lax.axis_size("seg")
    return mixer(
        n, segs, VALUE_HEADS // n, block_table, a_log, dt_bias, mixed_qkv, gate_z, gate_logits.T,
        conv_weight, norm_gain[None, :],
    )


def solution(mesh):
    return jax.shard_map(
        per_device,
        mesh=mesh,
        in_specs=(
            P(("seg", "cp"), None),
            P(("seg", "cp"), None),
            P(("seg", "cp"), None),
            P("seg", None),
            P(),
            P(),
            P(),
            P(),
        ),
        out_specs=P(("seg", "cp"), None),
        check_vma=False,
    )
```
